32 devices in a mesh: pair: 2 (over x), tp: 4 (over z), side: 4 (over y, core).
Axes of the slice: x: 2, y: 2, z: 4, core: 2. Of those that a mesh axis runs over, the one named last changes fastest.
Arguments:
- x_prompt: bfloat16 [2048, 4096], P(('pair', 'side')), parts along dimension 0
- s_len: int32 [8], P(('pair', 'side')), parts along dimension 0
- y_tok: bfloat16 [64, 4096], P(('pair', 'side')), parts along dimension 0
- k_cache: bfloat16 [1, 64, 256, 8, 4, 128], P(None, ('pair', 'side'), None, None, 'tp'), parts along dimension 1
- v_cache: bfloat16 [1, 64, 256, 8, 4, 128], P(None, ('pair', 'side'), None, None, 'tp'), parts along dimension 1
- c_len: int32 [64], P(('pair', 'side')), parts along dimension 0
- wqkv_a: bfloat16 [1, 4096, 32, 384], P(None, None, 'tp')
- wo_a: bfloat16 [1, 32, 128, 4096], P(None, 'tp')
- wug_a: bfloat16 [1, 4096, 2, 11008], P(None, None, None, 'tp')
- wd_a: bfloat16 [1, 11008, 4096], P(None, 'tp')
- norm_a: bfloat16 [1, 2, 4096], replicated
- wqkv_b: bfloat16 [1, 4096, 8, 4, 384], P(None, None, None, 'tp')
- wo_b: bfloat16 [1, 8, 4, 128, 4096], P(None, None, 'tp')
- wug_b: bfloat16 [1, 4096, 2, 11008], P(None, None, None, 'tp')
- wd_b: bfloat16 [1, 11008, 4096], P(None, 'tp')
- norm_b: bfloat16 [1, 2, 4096], replicated
Outputs:
- output 1: bfloat16 [2048, 4096], P(('pair', 'side')), parts along dimension 0
- output 2: bfloat16 [64, 4096], P(('pair', 'side')), parts along dimension 0
- output 3: bfloat16 [1, 2048, 8, 4, 128], P(None, ('pair', 'side'), None, 'tp'), parts along dimension 1
- output 4: bfloat16 [1, 2048, 8, 4, 128], P(None, ('pair', 'side'), None, 'tp'), parts along dimension 1
- output 5: bfloat16 [1, 64, 256, 8, 4, 128], P(None, ('pair', 'side'), None, None, 'tp'), parts along dimension 1
- output 6: bfloat16 [1, 64, 256, 8, 4, 128], P(None, ('pair', 'side'), None, None, 'tp'), parts along dimension 1
There are 2 independent parts. The reference program is written for one: setup_inputs(seed, part) draws one part's arguments, and reference() takes and returns one part's arrays. A program takes and returns all parts, laid end to end along the dimension named above; an argument that names none is the same for every part.
All inputs are finite; a program needn't handle non-finite values.
Results may differ from the reference program's by a relative error of at most 0.007746.
Values are sent between devices in bfloat16 or wider.
A program may use at most 1 GiB of HBM per device.

```python
import jax
import jax.numpy as jnp
from jax import lax

PROMPT = 256
DMODEL = 4096
Q_HEADS = 32
KV_HEADS = 32
HEAD_DIM = 128
FFN_DIM = 11008
LAYERS = 1
DEC_BATCH = 8
CACHE_LEN = 256
TP_SIZE = 4
NUM_SIDES = 4
KV_LOCAL = KV_HEADS // TP_SIZE
Q_GROUP = Q_HEADS // KV_HEADS
QKV_WIDTH = (Q_GROUP + 2) * HEAD_DIM
ROPE_BASE = 10000.0
NORM_EPS = 1e-5


def setup_inputs(seed: int = 0, part: int = 0) -> dict:
    weight_key, part_key = jax.random.split(jax.random.key(seed))
    wkeys = jax.random.split(weight_key, 10)
    pkeys = jax.random.split(jax.random.fold_in(part_key, part), 8)
    prompt_rows = NUM_SIDES * PROMPT
    batch_rows = NUM_SIDES * DEC_BATCH
    cache_shape = (LAYERS, batch_rows, CACHE_LEN, KV_LOCAL, TP_SIZE, HEAD_DIM)

    def normal_w(rkey, shape, fan_in):
        return (jax.random.normal(rkey, shape, jnp.float32) * fan_in ** -0.5).astype(jnp.bfloat16)

    def gain_draw(rkey):
        return (0.5 + jax.random.uniform(rkey, (LAYERS, 2, DMODEL), jnp.float32)).astype(jnp.bfloat16)

    lens_raw = jax.random.randint(pkeys[1], (NUM_SIDES,), 3 * PROMPT // 4, PROMPT + 1)
    full_at = jax.random.randint(pkeys[2], (), 0, NUM_SIDES)
    s_len = jnp.where(jnp.arange(NUM_SIDES) == full_at, PROMPT, lens_raw).astype(jnp.int32)
    ctx_raw = jax.random.randint(pkeys[6], (batch_rows,), CACHE_LEN // 2, CACHE_LEN)
    long_at = jax.random.randint(pkeys[7], (), 0, batch_rows)
    c_len = jnp.where(jnp.arange(batch_rows) == long_at, CACHE_LEN - 1, ctx_raw).astype(jnp.int32)
    return {
        'x_prompt': jax.random.normal(pkeys[0], (prompt_rows, DMODEL), jnp.float32).astype(jnp.bfloat16),
        's_len': s_len,
        'y_tok': jax.random.normal(pkeys[3], (batch_rows, DMODEL), jnp.float32).astype(jnp.bfloat16),
        'k_cache': jax.random.normal(pkeys[4], cache_shape, jnp.float32).astype(jnp.bfloat16),
        'v_cache': jax.random.normal(pkeys[5], cache_shape, jnp.float32).astype(jnp.bfloat16),
        'c_len': c_len,
        'wqkv_a': normal_w(wkeys[0], (LAYERS, DMODEL, KV_HEADS, QKV_WIDTH), DMODEL),
        'wo_a': normal_w(wkeys[1], (LAYERS, KV_HEADS, Q_GROUP * HEAD_DIM, DMODEL), Q_HEADS * HEAD_DIM),
        'wug_a': normal_w(wkeys[2], (LAYERS, DMODEL, 2, FFN_DIM), DMODEL),
        'wd_a': normal_w(wkeys[3], (LAYERS, FFN_DIM, DMODEL), FFN_DIM),
        'norm_a': gain_draw(wkeys[4]),
        'wqkv_b': normal_w(wkeys[5], (LAYERS, DMODEL, KV_LOCAL, TP_SIZE, QKV_WIDTH), DMODEL),
        'wo_b': normal_w(wkeys[6], (LAYERS, KV_LOCAL, TP_SIZE, Q_GROUP * HEAD_DIM, DMODEL), Q_HEADS * HEAD_DIM),
        'wug_b': normal_w(wkeys[7], (LAYERS, DMODEL, 2, FFN_DIM), DMODEL),
        'wd_b': normal_w(wkeys[8], (LAYERS, FFN_DIM, DMODEL), FFN_DIM),
        'norm_b': gain_draw(wkeys[9]),
    }


def rms_norm(hidden, gain):
    val_f32 = hidden.astype(jnp.float32)
    inv_rms = lax.rsqrt(jnp.mean(val_f32 * val_f32, axis=-1, keepdims=True) + NORM_EPS)
    return (val_f32 * inv_rms * gain.astype(jnp.float32)).astype(jnp.bfloat16)


def rope_rot(vals_in, positions):
    half_dim = vals_in.shape[-1] // 2
    inv_freq = ROPE_BASE ** (-jnp.arange(half_dim, dtype=jnp.float32) / half_dim)
    angles = positions.astype(jnp.float32)[:, None] * inv_freq[None, :]
    tab_shape = (angles.shape[0],) + (1,) * (vals_in.ndim - 2) + (half_dim,)
    cos_tab = jnp.cos(angles).reshape(tab_shape)
    sin_tab = jnp.sin(angles).reshape(tab_shape)
    lo_half = vals_in[..., :half_dim].astype(jnp.float32)
    hi_half = vals_in[..., half_dim:].astype(jnp.float32)
    return jnp.concatenate([lo_half * cos_tab - hi_half * sin_tab, hi_half * cos_tab + lo_half * sin_tab], axis=-1).astype(jnp.bfloat16)


def mlp_block(hidden, w_ug, w_down, gain):
    normed = rms_norm(hidden, gain)
    upgate = jnp.dot(normed, w_ug.reshape(DMODEL, 2 * FFN_DIM), preferred_element_type=jnp.float32).astype(jnp.bfloat16)
    upgate = upgate.reshape(hidden.shape[0], 2, FFN_DIM)
    act_out = (jax.nn.silu(upgate[:, 1].astype(jnp.float32)) * upgate[:, 0].astype(jnp.float32)).astype(jnp.bfloat16)
    mlp_down = jnp.dot(act_out, w_down, preferred_element_type=jnp.float32).astype(jnp.bfloat16)
    return (hidden.astype(jnp.float32) + mlp_down.astype(jnp.float32)).astype(jnp.bfloat16)


def prompt_layer(hidden, q_start, prev_k, prev_v, seq_len, w_qkv, w_out, w_ug, w_down, gain_pair):
    num_rows = hidden.shape[0]
    positions = q_start + jnp.arange(num_rows)
    normed = rms_norm(hidden, gain_pair[0])
    qkv_all = jnp.dot(normed, w_qkv.reshape(DMODEL, KV_HEADS * QKV_WIDTH), preferred_element_type=jnp.float32).astype(jnp.bfloat16)
    qkv_all = qkv_all.reshape(num_rows, KV_HEADS, Q_GROUP + 2, HEAD_DIM)
    queries = rope_rot(qkv_all[:, :, :Q_GROUP], positions)
    key_new = rope_rot(qkv_all[:, :, Q_GROUP], positions)
    val_new = qkv_all[:, :, Q_GROUP + 1]
    key_all = jnp.concatenate([prev_k, key_new], axis=0)
    val_all = jnp.concatenate([prev_v, val_new], axis=0)
    key_pos = jnp.arange(q_start + num_rows)
    allowed = (key_pos[None, :] <= positions[:, None]) & (key_pos[None, :] < seq_len)

    def head_attention(packed):
        q_head, k_head, v_head = packed
        scores = jnp.einsum('qgd,kd->gqk', q_head.astype(jnp.float32), k_head.astype(jnp.float32)) * HEAD_DIM ** -0.5
        scores = jnp.where(allowed[None], scores, -1e30)
        attn_prob = jax.nn.softmax(scores, axis=-1).astype(jnp.bfloat16)
        return jnp.einsum('gqk,kd->qgd', attn_prob.astype(jnp.float32), v_head.astype(jnp.float32)).astype(jnp.bfloat16)

    attn_out = lax.map(head_attention, (jnp.transpose(queries, (1, 0, 2, 3)), jnp.transpose(key_all, (1, 0, 2)), jnp.transpose(val_all, (1, 0, 2))))
    attn_out = jnp.transpose(attn_out, (1, 0, 2, 3)).reshape(num_rows, Q_HEADS * HEAD_DIM)
    attn_proj = jnp.dot(attn_out, w_out.reshape(Q_HEADS * HEAD_DIM, DMODEL), preferred_element_type=jnp.float32).astype(jnp.bfloat16)
    hidden = (hidden.astype(jnp.float32) + attn_proj.astype(jnp.float32)).astype(jnp.bfloat16)
    hidden = mlp_block(hidden, w_ug, w_down, gain_pair[1])
    return hidden, key_new, val_new


def prefill_side(x_rows, seq_len, wqkv_a, wo_a, wug_a, wd_a, norm_a):
    half_len = PROMPT // 2
    no_prev = jnp.zeros((0, KV_HEADS, HEAD_DIM), jnp.bfloat16)

    def first_step(hidden, layer_w):
        w_qkv, w_out, w_ug, w_down, gain_pair = layer_w
        hidden, key_new, val_new = prompt_layer(hidden, 0, no_prev, no_prev, seq_len, w_qkv, w_out, w_ug, w_down, gain_pair)
        return hidden, (key_new, val_new)

    def second_step(hidden, layer_w):
        w_qkv, w_out, w_ug, w_down, gain_pair, prev_k, prev_v = layer_w
        hidden, key_new, val_new = prompt_layer(hidden, half_len, prev_k, prev_v, seq_len, w_qkv, w_out, w_ug, w_down, gain_pair)
        return hidden, (key_new, val_new)

    weights = (wqkv_a, wo_a, wug_a, wd_a, norm_a)
    hidden_first, (keys_first, vals_first) = lax.scan(first_step, x_rows[:half_len], weights)
    hidden_second, (keys_second, vals_second) = lax.scan(second_step, x_rows[half_len:], weights + (keys_first, vals_first))
    valid = (jnp.arange(PROMPT) < seq_len)[None, :, None, None]
    key_cache = jnp.where(valid, jnp.concatenate([keys_first, keys_second], axis=1), 0.0).astype(jnp.bfloat16)
    val_cache = jnp.where(valid, jnp.concatenate([vals_first, vals_second], axis=1), 0.0).astype(jnp.bfloat16)
    return jnp.concatenate([hidden_first, hidden_second], axis=0), key_cache, val_cache


def decode_side(tokens, lengths, k_cache, v_cache, wqkv_b, wo_b, wug_b, wd_b, norm_b):
    slot_pos = jnp.arange(CACHE_LEN)
    write_slot = (slot_pos[None, :] == lengths[:, None])[:, :, None, None]

    def row_attention(packed):
        q_row, k_row, v_row, len_row = packed
        scores = jnp.einsum('hgd,thd->hgt', q_row.astype(jnp.float32), k_row.astype(jnp.float32)) * HEAD_DIM ** -0.5
        scores = jnp.where((slot_pos <= len_row)[None, None, :], scores, -1e30)
        attn_prob = jax.nn.softmax(scores, axis=-1).astype(jnp.bfloat16)
        return jnp.einsum('hgt,thd->hgd', attn_prob.astype(jnp.float32), v_row.astype(jnp.float32)).astype(jnp.bfloat16)

    def layer_step(hidden, layer_w):
        w_qkv, w_out, w_ug, w_down, gain_pair, cache_k, cache_v = layer_w
        normed = rms_norm(hidden, gain_pair[0])
        qkv_all = jnp.dot(normed, w_qkv.reshape(DMODEL, KV_HEADS * QKV_WIDTH), preferred_element_type=jnp.float32).astype(jnp.bfloat16)
        qkv_all = qkv_all.reshape(DEC_BATCH, KV_HEADS, Q_GROUP + 2, HEAD_DIM)
        queries = rope_rot(qkv_all[:, :, :Q_GROUP], lengths)
        key_new = rope_rot(qkv_all[:, :, Q_GROUP], lengths)
        val_new = qkv_all[:, :, Q_GROUP + 1]
        key_upd = jnp.where(write_slot, key_new[:, None], cache_k)
        val_upd = jnp.where(write_slot, val_new[:, None], cache_v)
        attn_out = lax.map(row_attention, (queries, key_upd, val_upd, lengths))
        attn_proj = jnp.dot(attn_out.reshape(DEC_BATCH, Q_HEADS * HEAD_DIM), w_out.reshape(Q_HEADS * HEAD_DIM, DMODEL), preferred_element_type=jnp.float32).astype(jnp.bfloat16)
        hidden = (hidden.astype(jnp.float32) + attn_proj.astype(jnp.float32)).astype(jnp.bfloat16)
        hidden = mlp_block(hidden, w_ug, w_down, gain_pair[1])
        return hidden, (key_upd, val_upd)

    hidden, (k_new, v_new) = lax.scan(layer_step, tokens, (wqkv_b, wo_b, wug_b, wd_b, norm_b, k_cache, v_cache))
    return hidden, k_new, v_new


def reference(x_prompt, s_len, y_tok, k_cache, v_cache, c_len, wqkv_a, wo_a, wug_a, wd_a, norm_a, wqkv_b, wo_b, wug_b, wd_b, norm_b):
    def one_prefill(packed):
        x_rows, seq_len = packed
        return prefill_side(x_rows, seq_len, wqkv_a, wo_a, wug_a, wd_a, norm_a)

    hidden_all, keys_all, vals_all = lax.map(one_prefill, (x_prompt.reshape(NUM_SIDES, PROMPT, DMODEL), s_len))

    def install(cache_all):
        moved = jnp.roll(cache_all, NUM_SIDES // 2, axis=0)
        return jnp.transpose(moved, (1, 0, 2, 3, 4)).reshape(LAYERS, NUM_SIDES * PROMPT, KV_LOCAL, TP_SIZE, HEAD_DIM)

    side_shape = (LAYERS, NUM_SIDES, DEC_BATCH, CACHE_LEN, KV_HEADS, HEAD_DIM)
    k_sides = jnp.transpose(k_cache.reshape(side_shape), (1, 0, 2, 3, 4, 5))
    v_sides = jnp.transpose(v_cache.reshape(side_shape), (1, 0, 2, 3, 4, 5))

    def one_decode(packed):
        tokens, lengths, cache_k, cache_v = packed
        return decode_side(tokens, lengths, cache_k, cache_v, wqkv_b, wo_b, wug_b, wd_b, norm_b)

    y_sides, k_new, v_new = lax.map(one_decode, (y_tok.reshape(NUM_SIDES, DEC_BATCH, DMODEL), c_len.reshape(NUM_SIDES, DEC_BATCH), k_sides, v_sides))
    out_shape = (LAYERS, NUM_SIDES * DEC_BATCH, CACHE_LEN, KV_LOCAL, TP_SIZE, HEAD_DIM)
    k_out = jnp.transpose(k_new, (1, 0, 2, 3, 4, 5)).reshape(out_shape)
    v_out = jnp.transpose(v_new, (1, 0, 2, 3, 4, 5)).reshape(out_shape)
    return (hidden_all.reshape(NUM_SIDES * PROMPT, DMODEL), y_sides.reshape(NUM_SIDES * DEC_BATCH, DMODEL), install(keys_all), install(vals_all), k_out, v_out)
```

```python
import jax
import jax.numpy as jnp
from jax import lax
from jax.experimental import pallas as pl
from jax.experimental.pallas import tpu as pltpu
from jax.sharding import PartitionSpec as P

ROPE_BASE = 10000.0
NORM_EPS = 1e-5


def rms_norm(hidden, gain):
    val_f32 = hidden.astype(jnp.float32)
    inv_rms = lax.rsqrt(jnp.mean(val_f32 * val_f32, axis=-1, keepdims=True) + NORM_EPS)
    return (val_f32 * inv_rms * gain.astype(jnp.float32)).astype(jnp.bfloat16)


def rope_rot(vals_in, positions):
    half_dim = vals_in.shape[-1] // 2
    inv_freq = ROPE_BASE ** (-jnp.arange(half_dim, dtype=jnp.float32) / half_dim)
    angles = positions.astype(jnp.float32)[:, None] * inv_freq[None, :]
    tab_shape = (angles.shape[0],) + (1,) * (vals_in.ndim - 2) + (half_dim,)
    cos_tab = jnp.cos(angles).reshape(tab_shape)
    sin_tab = jnp.sin(angles).reshape(tab_shape)
    lo_half = vals_in[..., :half_dim].astype(jnp.float32)
    hi_half = vals_in[..., half_dim:].astype(jnp.float32)
    return jnp.concatenate([lo_half * cos_tab - hi_half * sin_tab, hi_half * cos_tab + lo_half * sin_tab], axis=-1).astype(jnp.bfloat16)


MESH_ID = pl.DeviceIdType.MESH
COLS = 256
HALF_ROWS = 128
RING = 3
WIRE = 128
SKEW = 2


def block_kernel(x_ref, y_ref, attn_a_ref, attn_b_ref, norm_a_ref, norm_b_ref, wo_a, wug_a, wd_a, wo_b, wug_b, wd_b,
                 out_a, out_b,
                 part, rcv, hid, part_d, rcv_d, hid_d, normed, act, normed_d, act_d, ug_buf, dn_buf,
                 rs_send, rs_recv, ag_send, ag_recv, rsd_send, rsd_recv, agd_send, agd_recv, ug_sem, dn_sem, out_sem):
    ffn, width = wd_a.shape
    mid = width // 2
    per = mid // WIRE
    n_up = -(-ffn // COLS)
    last_up = ffn - COLS
    n_dn = width // 512
    z = lax.axis_index('tp')

    def pos(half):
        return half * z + (1 - half) * (3 - z)

    def fwd(half):
        return lax.rem(z + 4 + (2 * half - 1), 4)

    def bwd(half):
        return lax.rem(z + 4 - (2 * half - 1), 4)

    def remote(src, dst, ssem, rsem, target):
        return pltpu.make_async_remote_copy(src_ref=src, dst_ref=dst, send_sem=ssem, recv_sem=rsem,
                                            device_id={'tp': target}, device_id_type=MESH_ID)

    def rs_copy(half, g):
        return remote(part.at[half, g], rcv.at[half, g], rs_send.at[half], rs_recv.at[half, g], fwd(half))

    def ag_copy(half, g):
        return remote(hid.at[half, g], hid.at[half, g], ag_send.at[half], ag_recv.at[half, g], bwd(half))

    def rsd_copy(ar, half):
        return remote(part_d.at[ar, half], rcv_d.at[ar, half], rsd_send.at[ar, half], rsd_recv.at[ar, half], fwd(half))

    def agd_copy(ar, half):
        return remote(hid_d.at[ar, half], hid_d.at[ar, half], agd_send.at[ar, half], agd_recv.at[ar, half], bwd(half))

    def out_copy(half, g):
        row = (g // per - 2) * HALF_ROWS
        col = pl.multiple_of(half * mid + lax.rem(g, per) * WIRE, WIRE)
        return pltpu.make_async_copy(hid.at[half, g], out_a.at[pl.ds(pl.multiple_of(row, HALF_ROWS), HALF_ROWS), pl.ds(col, WIRE)], out_sem.at[half])

    def ug_copy(src, i, slot):
        row = pl.multiple_of(jnp.minimum(i * COLS, last_up), 64)
        return pltpu.make_async_copy(src.at[:, pl.ds(row, COLS), :], ug_buf.at[slot], ug_sem.at[slot])

    def dn_copy(src, j, slot):
        col = pl.multiple_of(lax.rem(j, 2) * mid + (j // 2) * 512, 512)
        return pltpu.make_async_copy(src.at[:, pl.ds(col, 512)], dn_buf.at[slot, pl.ds(0, src.shape[0]), :], dn_sem.at[slot])

    def slot_step(s, first, last, second, dec_at):
        ar = 1 if second else 0
        for half in range(2):
            where_at = pos(half)
            g = first + s - SKEW * where_at
            back = first + s - SKEW * (6 - where_at)
            dec = s - dec_at

            @pl.when((where_at == 0) & (g < last))
            def _():
                rs_copy(half, g).start()

            @pl.when((where_at > 0) & (where_at < 3) & (g >= first) & (g < last))
            def _():
                rs_copy(half, g).wait_recv()
                part[half, g] = part[half, g] + rcv[half, g]
                rs_copy(half, g).start()

            @pl.when((where_at == 3) & (g >= first) & (g < last))
            def _():
                rs_copy(half, g).wait_recv()
                total = (part[half, g] + rcv[half, g]).astype(jnp.bfloat16).astype(jnp.float32)
                if second:
                    base = hid[half, g - 2 * per]
                else:
                    row = pl.multiple_of((g // per) * HALF_ROWS, HALF_ROWS)
                    col = pl.multiple_of(half * mid + lax.rem(g, per) * WIRE, WIRE)
                    base = x_ref[pl.ds(row, HALF_ROWS), pl.ds(col, WIRE)]
                hid[half, g] = (base.astype(jnp.float32) + total).astype(jnp.bfloat16)
                ag_copy(half, g).start()
                if second:
                    out_copy(half, g).start()

            @pl.when((where_at < 3) & (back >= first) & (back < last))
            def _():
                ag_copy(half, back).wait_recv()

                @pl.when(where_at > 0)
                def _():
                    ag_copy(half, back).start()
                if second:
                    out_copy(half, back).start()

            @pl.when((where_at == 0) & (dec == 0))
            def _():
                rsd_copy(ar, half).start()

            @pl.when((where_at > 0) & (where_at < 3) & (dec == SKEW * where_at))
            def _():
                rsd_copy(ar, half).wait_recv()
                part_d[ar, half] = part_d[ar, half] + rcv_d[ar, half]
                rsd_copy(ar, half).start()

            @pl.when((where_at == 3) & (dec == SKEW * where_at))
            def _():
                rsd_copy(ar, half).wait_recv()
                total = (part_d[ar, half] + rcv_d[ar, half]).astype(jnp.bfloat16).astype(jnp.float32)
                base = hid_d[0, half] if ar else y_ref[:, half * mid:(half + 1) * mid]
                hid_d[ar, half] = (base.astype(jnp.float32) + total).astype(jnp.bfloat16)
                agd_copy(ar, half).start()

            @pl.when((where_at < 3) & (dec == SKEW * (6 - where_at)))
            def _():
                agd_copy(ar, half).wait_recv()

                @pl.when(where_at > 0)
                def _():
                    agd_copy(ar, half).start()

    def up_phase(src, nxt, base, lhs_ref, act_ref, comm):
        def step(i, carry):
            slot = lax.rem(base + i, RING)
            ug_copy(src, i, slot).wait()
            lhs = lhs_ref[...]
            dims = (((1,), (1,)), ((), ()))
            up = lax.dot_general(lhs, ug_buf[slot, 0], dims, preferred_element_type=jnp.float32).astype(jnp.bfloat16).astype(jnp.float32)
            gate = lax.dot_general(lhs, ug_buf[slot, 1], dims, preferred_element_type=jnp.float32).astype(jnp.bfloat16).astype(jnp.float32)
            val = jax.nn.silu(gate) * up
            col = lax.broadcasted_iota(jnp.int32, val.shape, 1) + jnp.minimum(i * COLS, last_up)
            act_ref[i] = jnp.where(col >= i * COLS, val, 0.0).astype(jnp.bfloat16)

            @pl.when(i + RING < n_up)
            def _():
                ug_copy(src, i + RING, slot).start()
            if nxt is not None:
                @pl.when(i + RING >= n_up)
                def _():
                    ug_copy(nxt, i + RING - n_up, slot).start()
            comm(i)
            return carry
        lax.fori_loop(0, n_up, step, 0)

    def dn_phase(src, nxt, base, compute, comm):
        def step(j, carry):
            slot = lax.rem(base + j, RING)
            dn_copy(src, j, slot).wait()
            compute(j, slot)

            @pl.when(j + RING < n_dn)
            def _():
                dn_copy(src, j + RING, slot).start()
            if nxt is not None:
                @pl.when(j + RING >= n_dn)
                def _():
                    dn_copy(nxt, j + RING - n_dn, slot).start()
            comm(j)
            return carry
        lax.fori_loop(0, n_dn, step, 0)

    def down_dot(act_ref, slot):
        total = None
        for i in range(n_up):
            start = min(i * COLS, last_up)
            piece = jnp.dot(act_ref[i], dn_buf[slot, start:start + COLS, :], preferred_element_type=jnp.float32)
            total = piece if total is None else total + piece
        return total

    def put_part(j, first, total):
        half = lax.rem(j, 2)
        for q in range(512 // WIRE):
            part[half, first + (j // 2) * (512 // WIRE) + q] = total[:, q * WIRE:(q + 1) * WIRE]

    def put_dec(ar, j, total):
        half = lax.rem(j, 2)
        part_d[ar, half, :, pl.ds(pl.multiple_of((j // 2) * 512, 512), 512)] = total

    def no_comm(i):
        pass

    def norm_rows(first):
        def square(q, acc):
            val = hid[q // per, first + lax.rem(q, per)].astype(jnp.float32)
            val = val * val
            return acc + val
        acc = lax.fori_loop(0, 2 * per, square, jnp.zeros((HALF_ROWS, WIRE), jnp.float32))
        inv = lax.rsqrt(jnp.sum(acc, axis=-1, keepdims=True) / width + NORM_EPS)

        def scale(q, carry):
            cols = pl.ds(pl.multiple_of(q * WIRE, WIRE), WIRE)
            val = hid[q // per, first + lax.rem(q, per)].astype(jnp.float32)
            normed[:, cols] = (val * inv * norm_a_ref[:, cols]).astype(jnp.bfloat16)
            return carry
        lax.fori_loop(0, 2 * per, scale, 0)

    barrier = pltpu.get_barrier_semaphore()
    for step in (-1, 1):
        @pl.when((z + step >= 0) & (z + step <= 3))
        def _():
            pl.semaphore_signal(barrier, inc=1, device_id={'tp': lax.rem(z + 4 + step, 4)}, device_id_type=MESH_ID)

    for slot in range(RING):
        dn_copy(wo_b, slot, slot).start()
    for slot in range(RING):
        ug_copy(wug_a, slot, slot).start()

    pl.semaphore_wait(barrier, jnp.where((z == 0) | (z == 3), 1, 2))

    def dec_proj(j, slot):
        put_dec(0, j, jnp.dot(attn_b_ref[...], dn_buf[slot, :attn_b_ref.shape[1], :], preferred_element_type=jnp.float32))
    dn_phase(wo_b, wo_a, 0, dec_proj, no_comm)

    def prompt_proj(j, slot):
        total = jnp.dot(attn_a_ref[...], dn_buf[slot, :attn_a_ref.shape[1], :], preferred_element_type=jnp.float32)
        put_part(j, 0, total[:HALF_ROWS])
        put_part(j, per, total[HALF_ROWS:])
    dn_phase(wo_a, wd_a, n_dn, prompt_proj, no_comm)

    depth = 6 * SKEW
    flow_one = (0, 2 * per, False, 0)
    dec_two = per + n_up + n_dn
    flow_c0 = (2 * per, 3 * per, True, dec_two)
    flow_c1 = (2 * per, 4 * per, True, dec_two)

    def slots(first, last, flow):
        def at(s, carry):
            slot_step(s, *flow)
            return carry
        lax.fori_loop(first, last, at, 0)

    def beside(first, count, flow):
        def at(i):
            @pl.when(i < count)
            def _():
                slot_step(first + i, *flow)
        return at

    slots(0, per + depth, flow_one)

    norm_rows(0)
    rest = per
    up_phase(wug_a, wug_a, 0, normed, act, beside(per + depth, n_up, flow_one))
    dn_phase(wd_a, wd_a, 2 * n_dn, lambda j, slot: put_part(j, 2 * per, down_dot(act, slot)), beside(per + depth + n_up, rest - n_up, flow_one))

    norm_rows(per)
    up_phase(wug_a, wug_b, n_up, normed, act, beside(0, n_up, flow_c0))
    dn_phase(wd_a, wd_b, 3 * n_dn, lambda j, slot: put_part(j, 3 * per, down_dot(act, slot)), beside(n_up, per - n_up, flow_c0))

    val = jnp.concatenate([hid_d[0, 0], hid_d[0, 1]], axis=-1).astype(jnp.float32)
    inv = lax.rsqrt(jnp.mean(val * val, axis=-1, keepdims=True) + NORM_EPS)
    normed_d[...] = (val * inv * norm_b_ref[...]).astype(jnp.bfloat16)
    up_phase(wug_b, None, 2 * n_up, normed_d, act_d, beside(per, n_up, flow_c1))
    dn_phase(wd_b, None, 4 * n_dn, lambda j, slot: put_dec(1, j, down_dot(act_d, slot)), beside(per + n_up, n_dn, flow_c1))
    slots(dec_two, max(2 * per, dec_two + 1) + depth, flow_c1)

    out_b[:, :mid] = hid_d[1, 0]
    out_b[:, mid:] = hid_d[1, 1]

    for half in range(2):
        for ar in range(2):
            @pl.when(pos(half) < 3)
            def _():
                rsd_copy(ar, half).wait_send()

            @pl.when(pos(half) > 0)
            def _():
                agd_copy(ar, half).wait_send()

    for half in range(2):
        @pl.when(pos(half) < 3)
        def _():
            remote(part.at[half], rcv.at[half], rs_send.at[half], rs_recv.at[half, 0], fwd(half)).wait_send()

        @pl.when(pos(half) > 0)
        def _():
            remote(hid.at[half], hid.at[half], ag_send.at[half], ag_recv.at[half, 0], bwd(half)).wait_send()
        pltpu.make_async_copy(hid.at[half, pl.ds(0, 2 * per)], hid.at[half, pl.ds(2 * per, 2 * per)], out_sem.at[half]).wait()


def block_call(x_rows, y_rows, attn_a, attn_b, norm_a, norm_b, wo_a, wug_a, wd_a, wo_b, wug_b, wd_b):
    rows, width = x_rows.shape
    dec_rows = y_rows.shape[0]
    ffn = wd_a.shape[0]
    mid = width // 2
    per = mid // WIRE
    n_up = -(-ffn // COLS)
    vmem = pl.BlockSpec(memory_space=pltpu.VMEM)
    hbm = pl.BlockSpec(memory_space=pl.ANY)
    dma = pltpu.SemaphoreType.DMA
    weights = 2 * (wo_a.size + wug_a.size + wd_a.size)
    return pl.pallas_call(
        block_kernel,
        out_shape=(jax.ShapeDtypeStruct((rows, width), jnp.bfloat16), jax.ShapeDtypeStruct((dec_rows, width), jnp.bfloat16)),
        in_specs=[vmem] * 6 + [hbm] * 6,
        out_specs=(hbm, vmem),
        scratch_shapes=[
            pltpu.VMEM((2, 4 * per, HALF_ROWS, WIRE), jnp.float32),
            pltpu.VMEM((2, 4 * per, HALF_ROWS, WIRE), jnp.float32),
            pltpu.VMEM((2, 4 * per, HALF_ROWS, WIRE), jnp.bfloat16),
            pltpu.VMEM((2, 2, dec_rows, mid), jnp.float32),
            pltpu.VMEM((2, 2, dec_rows, mid), jnp.float32),
            pltpu.VMEM((2, 2, dec_rows, mid), jnp.bfloat16),
            pltpu.VMEM((HALF_ROWS, width), jnp.bfloat16),
            pltpu.VMEM((n_up, HALF_ROWS, COLS), jnp.bfloat16),
            pltpu.VMEM((dec_rows, width), jnp.bfloat16),
            pltpu.VMEM((n_up, dec_rows, COLS), jnp.bfloat16),
            pltpu.VMEM((RING, 2, COLS, width), jnp.bfloat16),
            pltpu.VMEM((RING, ffn, 512), jnp.bfloat16),
            dma((2,)), dma((2, 4 * per)), dma((2,)), dma((2, 4 * per)),
            dma((2, 2)), dma((2, 2)), dma((2, 2)), dma((2, 2)),
            dma((RING,)), dma((RING,)), dma((2,)),
        ],
        compiler_params=pltpu.CompilerParams(collective_id=0, has_side_effects=True, vmem_limit_bytes=62 * 1024 * 1024),
        cost_estimate=pl.CostEstimate(flops=weights * (rows + dec_rows) // 2, bytes_accessed=weights * 3, transcendentals=0),
        name='block',
    )(x_rows, y_rows, attn_a, attn_b, norm_a, norm_b, wo_a, wug_a, wd_a, wo_b, wug_b, wd_b)


def prefill_attention(x_rows, seq_len, w_qkv, head_dim, gain):
    num_rows = x_rows.shape[0]
    kv_loc = w_qkv.shape[1]
    group = w_qkv.shape[2] // head_dim - 2
    positions = jnp.arange(num_rows)
    normed = rms_norm(x_rows, gain)
    qkv_all = jnp.einsum('sd,dhe->she', normed, w_qkv, preferred_element_type=jnp.float32).astype(jnp.bfloat16)
    qkv_all = qkv_all.reshape(num_rows, kv_loc, group + 2, head_dim)
    queries = rope_rot(qkv_all[:, :, :group], positions)
    keys = rope_rot(qkv_all[:, :, group], positions)
    vals = qkv_all[:, :, group + 1]
    allowed = (positions[None, :] <= positions[:, None]) & (positions[None, :] < seq_len)
    scores = jnp.einsum('qhgd,khd->hgqk', queries, keys, preferred_element_type=jnp.float32) * head_dim ** -0.5
    scores = jnp.where(allowed, scores, -1e30)
    attn_prob = jax.nn.softmax(scores, axis=-1).astype(jnp.bfloat16)
    attn_out = jnp.einsum('hgqk,khd->qhgd', attn_prob, vals, preferred_element_type=jnp.float32).astype(jnp.bfloat16)
    valid = (positions < seq_len)[:, None, None]
    zero_val = jnp.zeros((), jnp.bfloat16)
    return attn_out.reshape(num_rows, kv_loc * group * head_dim), jnp.where(valid, keys, zero_val), jnp.where(valid, vals, zero_val)


def decode_attention(tokens, lengths, k_cache, v_cache, w_qkv, head_dim, gain):
    batch_rows = tokens.shape[0]
    kv_loc = w_qkv.shape[1]
    tp_loc = w_qkv.shape[2]
    group = w_qkv.shape[3] // head_dim - 2
    slot_pos = jnp.arange(k_cache.shape[1])
    write_slot = (slot_pos[None, :] == lengths[:, None])[:, :, None, None, None]
    visible = (slot_pos[None, :] <= lengths[:, None])[:, None, None, None, :]
    normed = rms_norm(tokens, gain)
    qkv_all = jnp.einsum('bd,dije->bije', normed, w_qkv, preferred_element_type=jnp.float32).astype(jnp.bfloat16)
    qkv_all = qkv_all.reshape(batch_rows, kv_loc, tp_loc, group + 2, head_dim)
    queries = rope_rot(qkv_all[:, :, :, :group], lengths)
    key_new = rope_rot(qkv_all[:, :, :, group], lengths)
    val_new = qkv_all[:, :, :, group + 1]
    key_upd = jnp.where(write_slot, key_new[:, None], k_cache)
    val_upd = jnp.where(write_slot, val_new[:, None], v_cache)
    scores = jnp.einsum('bijge,bsije->bijgs', queries, key_upd, preferred_element_type=jnp.float32) * head_dim ** -0.5
    scores = jnp.where(visible, scores, -1e30)
    attn_prob = jax.nn.softmax(scores, axis=-1).astype(jnp.bfloat16)
    attn_out = jnp.einsum('bijgs,bsije->bijge', attn_prob, val_upd, preferred_element_type=jnp.float32).astype(jnp.bfloat16)
    return attn_out.reshape(batch_rows, kv_loc * tp_loc * group * head_dim), key_upd, val_upd


def hand_off(keys, vals, tp_size, side_size):
    num_rows, heads, head_dim = keys.shape
    fold = heads // tp_size
    both = jnp.stack([keys, vals]).reshape(2, num_rows, fold, tp_size, head_dim)
    tp_idx = lax.axis_index('tp')
    out = jnp.zeros((2, num_rows, tp_size, fold, head_dim), keys.dtype)
    for step in range(tp_size):
        piece = lax.dynamic_index_in_dim(both, (tp_idx + step) % tp_size, axis=3, keepdims=False)
        pairs = [(src * side_size + side, ((src + step) % tp_size) * side_size + (side + side_size // 2) % side_size)
                 for src in range(tp_size) for side in range(side_size)]
        moved = lax.ppermute(piece, ('tp', 'side'), pairs)
        out = lax.dynamic_update_index_in_dim(out, moved, (tp_idx - step) % tp_size, axis=2)
    out = out.reshape(2, 1, num_rows, heads, 1, head_dim)
    return out[0], out[1]


def solution(mesh):
    tp_size = mesh.shape['tp']
    side_size = mesh.shape['side']
    rows_spec = P(('pair', 'side'), None)
    flat_spec = P(('pair', 'side'))
    cache_spec = P(None, ('pair', 'side'), None, None, 'tp', None)
    prompt_spec = P(None, ('pair', 'side'), None, 'tp', None)
    in_specs = (rows_spec, flat_spec, rows_spec, cache_spec, cache_spec, flat_spec,
                P(None, None, 'tp', None), P(None, 'tp', None, None), P(None, None, None, 'tp'), P(None, 'tp', None), P(),
                P(None, None, None, 'tp', None), P(None, None, 'tp', None, None), P(None, None, None, 'tp'), P(None, 'tp', None), P())
    out_specs = (rows_spec, rows_spec, prompt_spec, prompt_spec, cache_spec, cache_spec)

    def body(x_prompt, s_len, y_tok, k_cache, v_cache, c_len, wqkv_a, wo_a, wug_a, wd_a, norm_a, wqkv_b, wo_b, wug_b, wd_b, norm_b):
        width = x_prompt.shape[1]
        head_dim = k_cache.shape[-1]
        attn_a, keys, vals = prefill_attention(x_prompt, s_len[0], wqkv_a[0], head_dim, norm_a[0, 0])
        k_prompt, v_prompt = hand_off(keys, vals, tp_size, side_size)
        attn_b, k_new, v_new = decode_attention(y_tok, c_len, k_cache[0], v_cache[0], wqkv_b[0], head_dim, norm_b[0, 0])
        hidden, y_out = block_call(
            x_prompt, y_tok, attn_a, attn_b, norm_a[0, 1:2].astype(jnp.float32), norm_b[0, 1:2].astype(jnp.float32),
            wo_a[0].reshape(-1, width), jnp.transpose(wug_a[0], (1, 2, 0)), wd_a[0],
            wo_b[0].reshape(-1, width), jnp.transpose(wug_b[0], (1, 2, 0)), wd_b[0])
        return hidden, y_out, k_prompt, v_prompt, k_new[None], v_new[None]

    return jax.shard_map(body, mesh=mesh, in_specs=in_specs, out_specs=out_specs, check_vma=False)
```

```python
import jax
import jax.numpy as jnp
from jax import lax
from jax.experimental import pallas as pl
from jax.experimental.pallas import tpu as pltpu
from jax.sharding import PartitionSpec as P

ROPE_BASE = 10000.0
NORM_EPS = 1e-5


def rms_norm(hidden, gain):
    val_f32 = hidden.astype(jnp.float32)
    inv_rms = lax.rsqrt(jnp.mean(val_f32 * val_f32, axis=-1, keepdims=True) + NORM_EPS)
    return (val_f32 * inv_rms * gain.astype(jnp.float32)).astype(jnp.bfloat16)


def rope_rot(vals_in, positions):
    half_dim = vals_in.shape[-1] // 2
    inv_freq = ROPE_BASE ** (-jnp.arange(half_dim, dtype=jnp.float32) / half_dim)
    angles = positions.astype(jnp.float32)[:, None] * inv_freq[None, :]
    tab_shape = (angles.shape[0],) + (1,) * (vals_in.ndim - 2) + (half_dim,)
    cos_tab = jnp.cos(angles).reshape(tab_shape)
    sin_tab = jnp.sin(angles).reshape(tab_shape)
    lo_half = vals_in[..., :half_dim].astype(jnp.float32)
    hi_half = vals_in[..., half_dim:].astype(jnp.float32)
    return jnp.concatenate([lo_half * cos_tab - hi_half * sin_tab, hi_half * cos_tab + lo_half * sin_tab], axis=-1).astype(jnp.bfloat16)


MESH_ID = pl.DeviceIdType.MESH
COLS = 256
HALF_ROWS = 128
RING = 3
WIRE = 128
FRONT_RING = 4
SKEW = 2


def block_kernel(x_ref, y_ref, attn_a_ref, attn_b_ref, norm_a_ref, norm_b_ref, wo_a, wug_a, wd_a, wo_b, wug_b, wd_b, keys, vals,
                 out_a, out_b, k_out, v_out,
                 part, rcv, hid, part_d, rcv_d, hid_d, normed, act, normed_d, act_d, ug_buf, dn_buf,
                 rs_send, rs_recv, ag_send, ag_recv, rsd_send, rsd_recv, agd_send, agd_recv, ug_sem, dn_sem, out_sem, hand_send, hand_recv):
    ffn, width = wd_a.shape
    mid = width // 2
    per = mid // WIRE
    n_up = -(-ffn // COLS)
    last_up = ffn - COLS
    n_dn = width // 512
    z = lax.axis_index('tp')

    def pos(half):
        return half * z + (1 - half) * (3 - z)

    def fwd(half):
        return lax.rem(z + 4 + (2 * half - 1), 4)

    def bwd(half):
        return lax.rem(z + 4 - (2 * half - 1), 4)

    def remote(src, dst, ssem, rsem, target):
        return pltpu.make_async_remote_copy(src_ref=src, dst_ref=dst, send_sem=ssem, recv_sem=rsem,
                                            device_id={'tp': target}, device_id_type=MESH_ID)

    def rs_copy(half, g):
        return remote(part.at[half, g], rcv.at[half, g], rs_send.at[half], rs_recv.at[half, g], fwd(half))

    def ag_copy(half, g):
        return remote(hid.at[half, g], hid.at[half, g], ag_send.at[half], ag_recv.at[half, g], bwd(half))

    def rsd_copy(ar, half):
        return remote(part_d.at[ar, half], rcv_d.at[ar, half], rsd_send.at[ar, half], rsd_recv.at[ar, half], fwd(half))

    def agd_copy(ar, half):
        return remote(hid_d.at[ar, half], hid_d.at[ar, half], agd_send.at[ar, half], agd_recv.at[ar, half], bwd(half))

    def out_copy(half, g):
        row = (g // per - 2) * HALF_ROWS
        col = pl.multiple_of(half * mid + lax.rem(g, per) * WIRE, WIRE)
        return pltpu.make_async_copy(hid.at[half, g], out_a.at[pl.ds(pl.multiple_of(row, HALF_ROWS), HALF_ROWS), pl.ds(col, WIRE)], out_sem.at[half])

    def ug_copy(src, i, slot):
        row = pl.multiple_of(jnp.minimum(i * COLS, last_up), 64)
        return pltpu.make_async_copy(src.at[:, pl.ds(row, COLS), :], ug_buf.at[slot], ug_sem.at[slot])

    def dn_copy(src, j, slot):
        col = pl.multiple_of(lax.rem(j, 2) * mid + (j // 2) * 512, 512)
        return pltpu.make_async_copy(src.at[:, pl.ds(col, 512)], dn_buf.at[slot, pl.ds(0, src.shape[0]), :], dn_sem.at[slot])

    def slot_step(s, first, last, second, dec_at):
        ar = 1 if second else 0
        for half in range(2):
            where_at = pos(half)
            g = first + s - SKEW * where_at
            back = first + s - SKEW * (6 - where_at)
            dec = s - dec_at

            @pl.when((where_at == 0) & (g < last))
            def _():
                rs_copy(half, g).start()

            @pl.when((where_at > 0) & (where_at < 3) & (g >= first) & (g < last))
            def _():
                rs_copy(half, g).wait_recv()
                part[half, g] = part[half, g] + rcv[half, g]
                rs_copy(half, g).start()

            @pl.when((where_at == 3) & (g >= first) & (g < last))
            def _():
                rs_copy(half, g).wait_recv()
                total = (part[half, g] + rcv[half, g]).astype(jnp.bfloat16).astype(jnp.float32)
                if second:
                    base = hid[half, g - 2 * per]
                else:
                    row = pl.multiple_of((g // per) * HALF_ROWS, HALF_ROWS)
                    col = pl.multiple_of(half * mid + lax.rem(g, per) * WIRE, WIRE)
                    base = x_ref[pl.ds(row, HALF_ROWS), pl.ds(col, WIRE)]
                hid[half, g] = (base.astype(jnp.float32) + total).astype(jnp.bfloat16)
                ag_copy(half, g).start()
                if second:
                    out_copy(half, g).start()

            @pl.when((where_at < 3) & (back >= first) & (back < last))
            def _():
                ag_copy(half, back).wait_recv()

                @pl.when(where_at > 0)
                def _():
                    ag_copy(half, back).start()
                if second:
                    out_copy(half, back).start()

            @pl.when((where_at == 0) & (dec == 0))
            def _():
                rsd_copy(ar, half).start()

            @pl.when((where_at > 0) & (where_at < 3) & (dec == SKEW * where_at))
            def _():
                rsd_copy(ar, half).wait_recv()
                part_d[ar, half] = part_d[ar, half] + rcv_d[ar, half]
                rsd_copy(ar, half).start()

            @pl.when((where_at == 3) & (dec == SKEW * where_at))
            def _():
                rsd_copy(ar, half).wait_recv()
                total = (part_d[ar, half] + rcv_d[ar, half]).astype(jnp.bfloat16).astype(jnp.float32)
                base = hid_d[0, half] if ar else y_ref[:, half * mid:(half + 1) * mid]
                hid_d[ar, half] = (base.astype(jnp.float32) + total).astype(jnp.bfloat16)
                agd_copy(ar, half).start()

            @pl.when((where_at < 3) & (dec == SKEW * (6 - where_at)))
            def _():
                agd_copy(ar, half).wait_recv()

                @pl.when(where_at > 0)
                def _():
                    agd_copy(ar, half).start()

    def up_phase(src, nxt, base, lhs_ref, act_ref, comm):
        def step(i, carry):
            slot = lax.rem(base + i, RING)
            ug_copy(src, i, slot).wait()
            lhs = lhs_ref[...]
            dims = (((1,), (1,)), ((), ()))
            up = lax.dot_general(lhs, ug_buf[slot, 0], dims, preferred_element_type=jnp.float32).astype(jnp.bfloat16).astype(jnp.float32)
            gate = lax.dot_general(lhs, ug_buf[slot, 1], dims, preferred_element_type=jnp.float32).astype(jnp.bfloat16).astype(jnp.float32)
            val = jax.nn.silu(gate) * up
            col = lax.broadcasted_iota(jnp.int32, val.shape, 1) + jnp.minimum(i * COLS, last_up)
            act_ref[i] = jnp.where(col >= i * COLS, val, 0.0).astype(jnp.bfloat16)

            @pl.when(i + RING < n_up)
            def _():
                ug_copy(src, i + RING, slot).start()
            if nxt is not None:
                @pl.when(i + RING >= n_up)
                def _():
                    ug_copy(nxt, i + RING - n_up, slot).start()
            comm(i)
            return carry
        lax.fori_loop(0, n_up, step, 0)

    def dn_phase(src, nxt, base, compute, comm):
        def step(j, carry):
            slot = lax.rem(base + j, RING)
            dn_copy(src, j, slot).wait()
            compute(j, slot)

            @pl.when(j + RING < n_dn)
            def _():
                dn_copy(src, j + RING, slot).start()
            if nxt is not None:
                @pl.when(j + RING >= n_dn)
                def _():
                    dn_copy(nxt, j + RING - n_dn, slot).start()
            comm(j)
            return carry
        lax.fori_loop(0, n_dn, step, 0)

    def down_dot(act_ref, slot):
        total = None
        for i in range(n_up):
            start = min(i * COLS, last_up)
            piece = jnp.dot(act_ref[i], dn_buf[slot, start:start + COLS, :], preferred_element_type=jnp.float32)
            total = piece if total is None else total + piece
        return total

    def put_part(j, first, total):
        half = lax.rem(j, 2)
        for q in range(512 // WIRE):
            part[half, first + (j // 2) * (512 // WIRE) + q] = total[:, q * WIRE:(q + 1) * WIRE]

    def put_dec(ar, j, total):
        half = lax.rem(j, 2)
        part_d[ar, half, :, pl.ds(pl.multiple_of((j // 2) * 512, 512), 512)] = total

    def no_comm(i):
        pass

    def norm_rows(first):
        def square(q, acc):
            val = hid[q // per, first + lax.rem(q, per)].astype(jnp.float32)
            val = val * val
            return acc + val
        acc = lax.fori_loop(0, 2 * per, square, jnp.zeros((HALF_ROWS, WIRE), jnp.float32))
        inv = lax.rsqrt(jnp.sum(acc, axis=-1, keepdims=True) / width + NORM_EPS)

        def scale(q, carry):
            cols = pl.ds(pl.multiple_of(q * WIRE, WIRE), WIRE)
            val = hid[q // per, first + lax.rem(q, per)].astype(jnp.float32)
            normed[:, cols] = (val * inv * norm_a_ref[:, cols]).astype(jnp.bfloat16)
            return carry
        lax.fori_loop(0, 2 * per, scale, 0)

    side = lax.axis_index('side')
    n_side = lax.axis_size('side')
    there = lax.rem(side + n_side // 2, n_side)

    def hand_copy(which, step):
        dest = lax.rem(z + step, 4)
        src, dst = ((keys, k_out), (vals, v_out))[which]
        fold = src.shape[2]
        return pltpu.make_async_remote_copy(
            src_ref=src.at[dest], dst_ref=dst.at[:, pl.ds(pl.multiple_of(z * fold, fold), fold)],
            send_sem=hand_send.at[which, step], recv_sem=hand_recv.at[which, step],
            device_id={'tp': dest, 'side': there}, device_id_type=MESH_ID)

    barrier = pltpu.get_barrier_semaphore()
    for step in range(4):
        pl.semaphore_signal(barrier, inc=1, device_id={'tp': lax.rem(z + step, 4), 'side': there}, device_id_type=MESH_ID)
    for step in (-1, 1):
        @pl.when((z + step >= 0) & (z + step <= 3))
        def _():
            pl.semaphore_signal(barrier, inc=1, device_id={'tp': lax.rem(z + 4 + step, 4)}, device_id_type=MESH_ID)

    for slot in range(RING):
        dn_copy(wo_b, slot, slot).start()
    for slot in range(RING):
        ug_copy(wug_a, slot, slot).start()

    pl.semaphore_wait(barrier, jnp.where((z == 0) | (z == 3), 5, 6))
    for step in range(4):
        hand_copy(0, step).start()

    def dec_proj(j, slot):
        put_dec(0, j, jnp.dot(attn_b_ref[...], dn_buf[slot, :attn_b_ref.shape[1], :], preferred_element_type=jnp.float32))
    dn_phase(wo_b, wo_a, 0, dec_proj, no_comm)

    def prompt_proj(j, slot):
        total = jnp.dot(attn_a_ref[...], dn_buf[slot, :attn_a_ref.shape[1], :], preferred_element_type=jnp.float32)
        put_part(j, 0, total[:HALF_ROWS])
        put_part(j, per, total[HALF_ROWS:])
    dn_phase(wo_a, wd_a, n_dn, prompt_proj, no_comm)

    depth = 6 * SKEW
    flow_one = (0, 2 * per, False, 0)
    dec_two = per + n_up + n_dn
    flow_c0 = (2 * per, 3 * per, True, dec_two)
    flow_c1 = (2 * per, 4 * per, True, dec_two)

    def slots(first, last, flow):
        def at(s, carry):
            slot_step(s, *flow)
            return carry
        lax.fori_loop(first, last, at, 0)

    def beside(first, count, flow):
        def at(i):
            @pl.when(i < count)
            def _():
                slot_step(first + i, *flow)
        return at

    slots(0, per + depth, flow_one)
    for step in range(4):
        hand_copy(1, step).start()

    norm_rows(0)
    lead = min(n_up, per)
    up_phase(wug_a, wug_a, 0, normed, act, beside(per + depth, lead, flow_one))
    dn_phase(wd_a, wd_a, 2 * n_dn, lambda j, slot: put_part(j, 2 * per, down_dot(act, slot)), beside(per + depth + lead, per - lead, flow_one))

    norm_rows(per)
    up_phase(wug_a, wug_b, n_up, normed, act, beside(0, lead, flow_c0))
    dn_phase(wd_a, wd_b, 3 * n_dn, lambda j, slot: put_part(j, 3 * per, down_dot(act, slot)), beside(lead, per - lead, flow_c0))

    val = jnp.concatenate([hid_d[0, 0], hid_d[0, 1]], axis=-1).astype(jnp.float32)
    inv = lax.rsqrt(jnp.mean(val * val, axis=-1, keepdims=True) + NORM_EPS)
    normed_d[...] = (val * inv * norm_b_ref[...]).astype(jnp.bfloat16)
    up_phase(wug_b, None, 2 * n_up, normed_d, act_d, beside(per, n_up, flow_c1))
    dn_phase(wd_b, None, 4 * n_dn, lambda j, slot: put_dec(1, j, down_dot(act_d, slot)), beside(per + n_up, n_dn, flow_c1))
    slots(dec_two, max(2 * per, dec_two + 1) + depth, flow_c1)

    for which in range(2):
        for step in range(4):
            hand_copy(which, step).wait()
    out_b[:, :mid] = hid_d[1, 0]
    out_b[:, mid:] = hid_d[1, 1]

    for half in range(2):
        for ar in range(2):
            @pl.when(pos(half) < 3)
            def _():
                rsd_copy(ar, half).wait_send()

            @pl.when(pos(half) > 0)
            def _():
                agd_copy(ar, half).wait_send()

    for half in range(2):
        @pl.when(pos(half) < 3)
        def _():
            remote(part.at[half], rcv.at[half], rs_send.at[half], rs_recv.at[half, 0], fwd(half)).wait_send()

        @pl.when(pos(half) > 0)
        def _():
            remote(hid.at[half], hid.at[half], ag_send.at[half], ag_recv.at[half, 0], bwd(half)).wait_send()
        pltpu.make_async_copy(hid.at[half, pl.ds(0, 2 * per)], hid.at[half, pl.ds(2 * per, 2 * per)], out_sem.at[half]).wait()


def block_call(x_rows, y_rows, attn_a, attn_b, norm_a, norm_b, wo_a, wug_a, wd_a, wo_b, wug_b, wd_b, keys, vals):
    rows, width = x_rows.shape
    dec_rows = y_rows.shape[0]
    ffn = wd_a.shape[0]
    mid = width // 2
    per = mid // WIRE
    n_up = -(-ffn // COLS)
    vmem = pl.BlockSpec(memory_space=pltpu.VMEM)
    hbm = pl.BlockSpec(memory_space=pl.ANY)
    dma = pltpu.SemaphoreType.DMA
    weights = 2 * (wo_a.size + wug_a.size + wd_a.size)
    return pl.pallas_call(
        block_kernel,
        out_shape=(jax.ShapeDtypeStruct((rows, width), jnp.bfloat16), jax.ShapeDtypeStruct((dec_rows, width), jnp.bfloat16),
                   *[jax.ShapeDtypeStruct((rows, keys.shape[0] * keys.shape[2]), jnp.bfloat16)] * 2),
        in_specs=[vmem] * 6 + [hbm] * 8,
        out_specs=(hbm, vmem, hbm, hbm),
        scratch_shapes=[
            pltpu.VMEM((2, 4 * per, HALF_ROWS, WIRE), jnp.float32),
            pltpu.VMEM((2, 4 * per, HALF_ROWS, WIRE), jnp.float32),
            pltpu.VMEM((2, 4 * per, HALF_ROWS, WIRE), jnp.bfloat16),
            pltpu.VMEM((2, 2, dec_rows, mid), jnp.float32),
            pltpu.VMEM((2, 2, dec_rows, mid), jnp.float32),
            pltpu.VMEM((2, 2, dec_rows, mid), jnp.bfloat16),
            pltpu.VMEM((HALF_ROWS, width), jnp.bfloat16),
            pltpu.VMEM((n_up, HALF_ROWS, COLS), jnp.bfloat16),
            pltpu.VMEM((dec_rows, width), jnp.bfloat16),
            pltpu.VMEM((n_up, dec_rows, COLS), jnp.bfloat16),
            pltpu.VMEM((RING, 2, COLS, width), jnp.bfloat16),
            pltpu.VMEM((RING, ffn, 512), jnp.bfloat16),
            dma((2,)), dma((2, 4 * per)), dma((2,)), dma((2, 4 * per)),
            dma((2, 2)), dma((2, 2)), dma((2, 2)), dma((2, 2)),
            dma((RING,)), dma((RING,)), dma((2,)), dma((2, 4)), dma((2, 4)),
        ],
        compiler_params=pltpu.CompilerParams(collective_id=0, has_side_effects=True, vmem_limit_bytes=62 * 1024 * 1024),
        cost_estimate=pl.CostEstimate(flops=weights * (rows + dec_rows) // 2, bytes_accessed=weights * 3, transcendentals=0),
        name='block',
    )(x_rows, y_rows, attn_a, attn_b, norm_a, norm_b, wo_a, wug_a, wd_a, wo_b, wug_b, wd_b, keys, vals)


def front_kernel(s_len, c_len, qkv_a, cos_a, sin_a, slices_b, cos_b, sin_b, wqkv_b, k_cache, v_cache,
                 attn_a, keys, vals, attn_b, k_new, v_new,
                 k_buf, v_buf, w_buf, spread, acc, rows_b, k_in, v_in, k_sem, v_sem, w_sem):
    heads, rows, _ = qkv_a.shape
    head_dim = cos_a.shape[1]
    half = head_dim // 2
    dec_rows, slots_heads, _ = k_cache.shape
    n_tp = keys.shape[0]
    depth = w_buf.shape[1]
    n_w = wqkv_b.shape[0] // depth
    scale = head_dim ** -0.5

    def w_copy(i, slot):
        return pltpu.make_async_copy(wqkv_b.at[pl.ds(pl.multiple_of(i * depth, depth), depth), :], w_buf.at[slot], w_sem.at[slot])

    for slot in range(FRONT_RING):
        w_copy(slot, slot).start()

    def cache_in(b, carry):
        pltpu.make_async_copy(k_cache.at[b], k_buf.at[b], k_in.at[b]).start()
        pltpu.make_async_copy(v_cache.at[b], v_buf.at[b], v_in.at[b]).start()
        return carry
    lax.fori_loop(0, dec_rows, cache_in, 0)

    def rotate(val, cos_tab, sin_tab):
        val = val.astype(jnp.float32)
        swapped = jnp.concatenate([val[:, half:], val[:, :half]], axis=-1)
        return (val * cos_tab + swapped * sin_tab).astype(jnp.bfloat16)

    row = lax.broadcasted_iota(jnp.int32, (rows, rows), 0)
    col = lax.broadcasted_iota(jnp.int32, (rows, rows), 1)
    allowed = (col <= row) & (col < s_len[0])
    valid = lax.broadcasted_iota(jnp.int32, (rows, head_dim), 0) < s_len[0]
    zero = jnp.zeros((rows, head_dim), jnp.float32)
    dims = (((1,), (1,)), ((), ()))
    for h in range(heads):
        query = rotate(qkv_a[h, :, :head_dim], cos_a[...], sin_a[...])
        key = rotate(qkv_a[h, :, head_dim:2 * head_dim], cos_a[...], sin_a[...])
        val = qkv_a[h, :, 2 * head_dim:]
        place = pl.ds((h // n_tp) * head_dim, head_dim)
        keys[h % n_tp, :, place] = jnp.where(valid, key.astype(jnp.float32), zero).astype(jnp.bfloat16)
        vals[h % n_tp, :, place] = jnp.where(valid, val.astype(jnp.float32), zero).astype(jnp.bfloat16)
        scores = lax.dot_general(query, key, dims, preferred_element_type=jnp.float32) * scale
        scores = jnp.where(allowed, scores, -1e30)
        expd = jnp.exp(scores - jnp.max(scores, axis=-1, keepdims=True))
        prob = (expd / jnp.sum(expd, axis=-1, keepdims=True)).astype(jnp.bfloat16)
        attn_a[:, h * head_dim:(h + 1) * head_dim] = jnp.dot(prob, val, preferred_element_type=jnp.float32).astype(jnp.bfloat16)

    lanes = spread.shape[1]
    span = lanes // heads
    one = (lax.broadcasted_iota(jnp.int32, (span, lanes), 1) // heads == lax.broadcasted_iota(jnp.int32, (span, lanes), 0))
    spread[...] = jnp.dot(slices_b[...], jnp.where(one, 1.0, 0.0).astype(jnp.bfloat16), preferred_element_type=jnp.float32)
    own = lax.broadcasted_iota(jnp.int32, (dec_rows, heads, lanes), 2) % heads == lax.broadcasted_iota(jnp.int32, (dec_rows, heads, lanes), 1)
    acc[...] = jnp.zeros_like(acc)
    inner = depth // lanes

    def project(i, carry):
        slot = lax.rem(i, FRONT_RING)
        w_copy(i, slot).wait()
        total = acc[...]
        for j in range(inner):
            part = spread[pl.ds(pl.multiple_of((i * inner + j) * dec_rows, dec_rows), dec_rows), :]
            wide = jnp.where(own, jnp.broadcast_to(part[:, None, :], own.shape), 0.0).reshape(dec_rows * heads, lanes)
            total = total + jnp.dot(wide.astype(jnp.bfloat16), w_buf[slot, j * lanes:(j + 1) * lanes, :], preferred_element_type=jnp.float32)
        acc[...] = total

        @pl.when(i + FRONT_RING < n_w)
        def _():
            w_copy(i + FRONT_RING, slot).start()
        return carry
    lax.fori_loop(0, n_w, project, 0)

    proj = acc[...].astype(jnp.bfloat16)
    rows_b[0] = rotate(proj[:, :head_dim], cos_b[...], sin_b[...]).astype(jnp.float32)
    rows_b[1] = rotate(proj[:, head_dim:2 * head_dim], cos_b[...], sin_b[...]).astype(jnp.float32)
    rows_b[2] = proj[:, 2 * head_dim:].astype(jnp.float32)

    slot_of = lax.broadcasted_iota(jnp.int32, (slots_heads, head_dim), 0) // heads
    pair = lax.broadcasted_iota(jnp.int32, (heads, slots_heads), 1)
    same = pair % heads == lax.broadcasted_iota(jnp.int32, (heads, slots_heads), 0)

    def attend(b, carry):
        length = c_len[b]
        mine = pl.ds(pl.multiple_of(b * heads, heads), heads)

        def updated(buf, new):
            wide = jnp.broadcast_to(new[None], (slots_heads // heads, heads, head_dim)).reshape(slots_heads, head_dim)
            return jnp.where(slot_of == length, wide, buf[b].astype(jnp.float32)).astype(jnp.bfloat16)
        pltpu.make_async_copy(k_cache.at[b], k_buf.at[b], k_in.at[b]).wait()
        k_buf[b] = updated(k_buf, rows_b[1, mine])
        pltpu.make_async_copy(v_cache.at[b], v_buf.at[b], v_in.at[b]).wait()
        v_buf[b] = updated(v_buf, rows_b[2, mine])
        pltpu.make_async_copy(k_buf.at[b], k_new.at[b], k_sem.at[b]).start()
        pltpu.make_async_copy(v_buf.at[b], v_new.at[b], v_sem.at[b]).start()
        scores = lax.dot_general(rows_b[0, mine].astype(jnp.bfloat16), k_buf[b], dims, preferred_element_type=jnp.float32) * scale
        scores = jnp.where(same & (pair // heads <= length), scores, -1e30)
        expd = jnp.exp(scores - jnp.max(scores, axis=-1, keepdims=True))
        prob = (expd / jnp.sum(expd, axis=-1, keepdims=True)).astype(jnp.bfloat16)
        attn_b[b] = jnp.dot(prob, v_buf[b], preferred_element_type=jnp.float32).astype(jnp.bfloat16)
        return carry
    lax.fori_loop(0, dec_rows, attend, 0)

    def cache_out(b, carry):
        pltpu.make_async_copy(k_buf.at[b], k_new.at[b], k_sem.at[b]).wait()
        pltpu.make_async_copy(v_buf.at[b], v_new.at[b], v_sem.at[b]).wait()
        return carry
    lax.fori_loop(0, dec_rows, cache_out, 0)


def rope_tables(positions, head_dim):
    half_dim = head_dim // 2
    inv_freq = ROPE_BASE ** (-jnp.arange(half_dim, dtype=jnp.float32) / half_dim)
    angles = positions.astype(jnp.float32)[:, None] * inv_freq[None, :]
    cos_tab, sin_tab = jnp.cos(angles), jnp.sin(angles)
    return jnp.concatenate([cos_tab, cos_tab], axis=-1), jnp.concatenate([-sin_tab, sin_tab], axis=-1)


def front_call(x_rows, y_rows, s_len, c_len, w_qkv_a, w_qkv_b, gain_a, gain_b, k_cache, v_cache, tp_size):
    num_rows, width = x_rows.shape
    dec_rows = y_rows.shape[0]
    heads, wide = w_qkv_a.shape[1:]
    head_dim = k_cache.shape[-1]
    cache_rows = k_cache.shape[1] * heads
    qkv_a = jnp.einsum('sd,dhe->she', rms_norm(x_rows, gain_a), w_qkv_a, preferred_element_type=jnp.float32).astype(jnp.bfloat16)
    qkv_a = jnp.transpose(qkv_a, (1, 0, 2))
    lanes = 256
    span = lanes // heads
    slices_b = jnp.transpose(rms_norm(y_rows, gain_b).reshape(dec_rows, width // span, span), (1, 0, 2)).reshape(-1, span)
    cos_a, sin_a = rope_tables(jnp.arange(num_rows), head_dim)
    cos_b, sin_b = (jnp.repeat(tab, heads, axis=0) for tab in rope_tables(c_len, head_dim))
    vmem = pl.BlockSpec(memory_space=pltpu.VMEM)
    smem = pl.BlockSpec(memory_space=pltpu.SMEM)
    hbm = pl.BlockSpec(memory_space=pl.ANY)
    dma = pltpu.SemaphoreType.DMA
    depth = 2048
    fold = heads // tp_size * head_dim
    bf16 = jnp.bfloat16
    cache = jax.ShapeDtypeStruct((dec_rows, cache_rows, head_dim), bf16)
    moved = jax.ShapeDtypeStruct((tp_size, num_rows, fold), bf16)
    return pl.pallas_call(
        front_kernel,
        out_shape=(jax.ShapeDtypeStruct((num_rows, heads * head_dim), bf16), moved, moved,
                   jax.ShapeDtypeStruct((dec_rows, heads, head_dim), bf16), cache, cache),
        in_specs=[smem] * 2 + [vmem] * 6 + [hbm] * 3,
        out_specs=(vmem, vmem, vmem, vmem, hbm, hbm),
        scratch_shapes=[
            pltpu.VMEM((dec_rows, cache_rows, head_dim), bf16),
            pltpu.VMEM((dec_rows, cache_rows, head_dim), bf16),
            pltpu.VMEM((FRONT_RING, depth, wide), bf16),
            pltpu.VMEM((width // span * dec_rows, lanes), jnp.float32),
            pltpu.VMEM((dec_rows * heads, wide), jnp.float32),
            pltpu.VMEM((3, dec_rows * heads, head_dim), jnp.float32),
            dma((dec_rows,)), dma((dec_rows,)), dma((dec_rows,)), dma((dec_rows,)), dma((FRONT_RING,)),
        ],
        compiler_params=pltpu.CompilerParams(vmem_limit_bytes=40 * 1024 * 1024),
        cost_estimate=pl.CostEstimate(flops=2 * width * heads * wide * dec_rows, bytes_accessed=60000000, transcendentals=0),
        name='front',
    )(s_len, c_len, qkv_a, cos_a, sin_a, slices_b, cos_b, sin_b, w_qkv_b.reshape(width * heads, wide),
      k_cache.reshape(dec_rows, cache_rows, head_dim), v_cache.reshape(dec_rows, cache_rows, head_dim))


def solution(mesh):
    tp_size = mesh.shape['tp']
    side_size = mesh.shape['side']
    rows_spec = P(('pair', 'side'), None)
    flat_spec = P(('pair', 'side'))
    cache_spec = P(None, ('pair', 'side'), None, None, 'tp', None)
    prompt_spec = P(None, ('pair', 'side'), None, 'tp', None)
    in_specs = (rows_spec, flat_spec, rows_spec, cache_spec, cache_spec, flat_spec,
                P(None, None, 'tp', None), P(None, 'tp', None, None), P(None, None, None, 'tp'), P(None, 'tp', None), P(),
                P(None, None, None, 'tp', None), P(None, None, 'tp', None, None), P(None, None, None, 'tp'), P(None, 'tp', None), P())
    out_specs = (rows_spec, rows_spec, prompt_spec, prompt_spec, cache_spec, cache_spec)

    def body(x_prompt, s_len, y_tok, k_cache, v_cache, c_len, wqkv_a, wo_a, wug_a, wd_a, norm_a, wqkv_b, wo_b, wug_b, wd_b, norm_b):
        width = x_prompt.shape[1]
        head_dim = k_cache.shape[-1]
        dec_rows, slots, heads = k_cache.shape[1:4]
        attn_a, keys, vals, attn_b, k_new, v_new = front_call(
            x_prompt, y_tok, s_len, c_len, wqkv_a[0], wqkv_b[0, :, :, 0], norm_a[0, 0], norm_b[0, 0],
            k_cache[0, :, :, :, 0], v_cache[0, :, :, :, 0], tp_size)
        hidden, y_out, k_prompt, v_prompt = block_call(
            x_prompt, y_tok, attn_a, attn_b.reshape(dec_rows, -1), norm_a[0, 1:2].astype(jnp.float32), norm_b[0, 1:2].astype(jnp.float32),
            wo_a[0].reshape(-1, width), jnp.transpose(wug_a[0], (1, 2, 0)), wd_a[0],
            wo_b[0].reshape(-1, width), jnp.transpose(wug_b[0], (1, 2, 0)), wd_b[0], keys, vals)
        prompt_shape = (1, x_prompt.shape[0], heads, 1, head_dim)
        return (hidden, y_out, k_prompt.reshape(prompt_shape), v_prompt.reshape(prompt_shape),
                k_new.reshape(k_cache.shape), v_new.reshape(v_cache.shape))

    return jax.shard_map(body, mesh=mesh, in_specs=in_specs, out_specs=out_specs, check_vma=False)
```

```python
import jax
import jax.numpy as jnp
from jax import lax
from jax.experimental import pallas as pl
from jax.experimental.pallas import tpu as pltpu
from jax.sharding import PartitionSpec as P

ROPE_BASE = 10000.0
NORM_EPS = 1e-5


def rms_norm(hidden, gain):
    val_f32 = hidden.astype(jnp.float32)
    inv_rms = lax.rsqrt(jnp.mean(val_f32 * val_f32, axis=-1, keepdims=True) + NORM_EPS)
    return (val_f32 * inv_rms * gain.astype(jnp.float32)).astype(jnp.bfloat16)


def rope_rot(vals_in, positions):
    half_dim = vals_in.shape[-1] // 2
    inv_freq = ROPE_BASE ** (-jnp.arange(half_dim, dtype=jnp.float32) / half_dim)
    angles = positions.astype(jnp.float32)[:, None] * inv_freq[None, :]
    tab_shape = (angles.shape[0],) + (1,) * (vals_in.ndim - 2) + (half_dim,)
    cos_tab = jnp.cos(angles).reshape(tab_shape)
    sin_tab = jnp.sin(angles).reshape(tab_shape)
    lo_half = vals_in[..., :half_dim].astype(jnp.float32)
    hi_half = vals_in[..., half_dim:].astype(jnp.float32)
    return jnp.concatenate([lo_half * cos_tab - hi_half * sin_tab, hi_half * cos_tab + lo_half * sin_tab], axis=-1).astype(jnp.bfloat16)


MESH_ID = pl.DeviceIdType.MESH
COLS = 256
HALF_ROWS = 128
RING = 3
WIRE = 128
WIRE_ROWS = 128
FRONT_RING = 4
SKEW = 3
RATE = 1


def block_kernel(x_ref, y_ref, attn_a_ref, attn_b_ref, norm_a_ref, norm_b_ref, wo_a, wug_a, wd_a, wo_b, wug_b, wd_b, keys, vals,
                 out_a, out_b, k_out, v_out,
                 part, rcv, hid, part_d, rcv_d, hid_d, normed, act, normed_d, act_d, ug_buf, dn_buf,
                 rs_send, rs_recv, ag_send, ag_recv, rsd_send, rsd_recv, agd_send, agd_recv, ug_sem, dn_sem, out_sem, hand_send, hand_recv):
    ffn, width = wd_a.shape
    mid = width // 2
    cuts = HALF_ROWS // WIRE_ROWS
    per = mid // WIRE * cuts
    n_up = -(-ffn // COLS)
    last_up = ffn - COLS
    n_dn = width // 512
    z = lax.axis_index('tp')

    def pos(half):
        return half * z + (1 - half) * (3 - z)

    def fwd(half):
        return lax.rem(z + 4 + (2 * half - 1), 4)

    def bwd(half):
        return lax.rem(z + 4 - (2 * half - 1), 4)

    def remote(src, dst, ssem, rsem, target):
        return pltpu.make_async_remote_copy(src_ref=src, dst_ref=dst, send_sem=ssem, recv_sem=rsem,
                                            device_id={'tp': target}, device_id_type=MESH_ID)

    def rs_copy(half, g):
        return remote(part.at[half, g], rcv.at[half, g], rs_send.at[half], rs_recv.at[half, g], fwd(half))

    def ag_copy(half, g):
        return remote(hid.at[half, g], hid.at[half, g], ag_send.at[half], ag_recv.at[half, g], bwd(half))

    def rsd_copy(ar, half):
        return remote(part_d.at[ar, half], rcv_d.at[ar, half], rsd_send.at[ar, half], rsd_recv.at[ar, half], fwd(half))

    def agd_copy(ar, half):
        return remote(hid_d.at[ar, half], hid_d.at[ar, half], agd_send.at[ar, half], agd_recv.at[ar, half], bwd(half))

    def place(half, g):
        row = (lax.rem(g // per, 2) * cuts + lax.rem(g, cuts)) * WIRE_ROWS
        col = half * mid + lax.rem(g, per) // cuts * WIRE
        return pl.ds(pl.multiple_of(row, WIRE_ROWS), WIRE_ROWS), pl.ds(pl.multiple_of(col, WIRE), WIRE)

    def out_copy(half, g):
        return pltpu.make_async_copy(hid.at[half, g], out_a.at[place(half, g)], out_sem.at[half])

    def ug_copy(src, i, slot):
        row = pl.multiple_of(jnp.minimum(i * COLS, last_up), 64)
        return pltpu.make_async_copy(src.at[:, pl.ds(row, COLS), :], ug_buf.at[slot], ug_sem.at[slot])

    def dn_copy(src, j, slot):
        col = pl.multiple_of(lax.rem(j, 2) * mid + (j // 2) * 512, 512)
        return pltpu.make_async_copy(src.at[:, pl.ds(col, 512)], dn_buf.at[slot, pl.ds(0, src.shape[0]), :], dn_sem.at[slot])

    def slot_step(s, first, last, second, dec_at):
        ar = 1 if second else 0
        if not second:
            for which in range(2):
                turn = s - hand_at - 8 * which

                @pl.when((turn >= 0) & (turn < 8) & (lax.rem(turn, 2) == 0))
                def _():
                    hand_copy(which, turn // 2).start()

        for half in range(2):
            where_at = pos(half)
            g = first + s - SKEW * where_at
            back = first + s - SKEW * (6 - where_at)
            dec = s - dec_at

            @pl.when((where_at == 0) & (g < last))
            def _():
                rs_copy(half, g).start()

            @pl.when((where_at > 0) & (where_at < 3) & (g >= first) & (g < last))
            def _():
                rs_copy(half, g).wait_recv()
                part[half, g] = part[half, g] + rcv[half, g]
                rs_copy(half, g).start()

            @pl.when((where_at == 3) & (g >= first) & (g < last))
            def _():
                rs_copy(half, g).wait_recv()
                total = (part[half, g] + rcv[half, g]).astype(jnp.bfloat16).astype(jnp.float32)
                if second:
                    base = hid[half, g - 2 * per]
                else:
                    base = x_ref[place(half, g)]
                hid[half, g] = (base.astype(jnp.float32) + total).astype(jnp.bfloat16)
                ag_copy(half, g).start()
                if second:
                    out_copy(half, g).start()

            @pl.when((where_at < 3) & (back >= first) & (back < last))
            def _():
                ag_copy(half, back).wait_recv()

                @pl.when(where_at > 0)
                def _():
                    ag_copy(half, back).start()
                if second:
                    out_copy(half, back).start()

            @pl.when((where_at == 0) & (dec == 0))
            def _():
                rsd_copy(ar, half).start()

            @pl.when((where_at > 0) & (where_at < 3) & (dec == SKEW * where_at))
            def _():
                rsd_copy(ar, half).wait_recv()
                part_d[ar, half] = part_d[ar, half] + rcv_d[ar, half]
                rsd_copy(ar, half).start()

            @pl.when((where_at == 3) & (dec == SKEW * where_at))
            def _():
                rsd_copy(ar, half).wait_recv()
                total = (part_d[ar, half] + rcv_d[ar, half]).astype(jnp.bfloat16).astype(jnp.float32)
                base = hid_d[0, half] if ar else y_ref[:, half * mid:(half + 1) * mid]
                hid_d[ar, half] = (base.astype(jnp.float32) + total).astype(jnp.bfloat16)
                agd_copy(ar, half).start()

            @pl.when((where_at < 3) & (dec == SKEW * (6 - where_at)))
            def _():
                agd_copy(ar, half).wait_recv()

                @pl.when(where_at > 0)
                def _():
                    agd_copy(ar, half).start()

    def up_phase(src, nxt, base, lhs_ref, act_ref, comm):
        def step(i, carry):
            slot = lax.rem(base + i, RING)
            ug_copy(src, i, slot).wait()
            lhs = lhs_ref[...]
            dims = (((1,), (1,)), ((), ()))
            up = lax.dot_general(lhs, ug_buf[slot, 0], dims, preferred_element_type=jnp.float32).astype(jnp.bfloat16).astype(jnp.float32)
            gate = lax.dot_general(lhs, ug_buf[slot, 1], dims, preferred_element_type=jnp.float32).astype(jnp.bfloat16).astype(jnp.float32)
            val = jax.nn.silu(gate) * up
            col = lax.broadcasted_iota(jnp.int32, val.shape, 1) + jnp.minimum(i * COLS, last_up)
            act_ref[i] = jnp.where(col >= i * COLS, val, 0.0).astype(jnp.bfloat16)

            @pl.when(i + RING < n_up)
            def _():
                ug_copy(src, i + RING, slot).start()
            if nxt is not None:
                @pl.when(i + RING >= n_up)
                def _():
                    ug_copy(nxt, i + RING - n_up, slot).start()
            comm(i)
            return carry
        lax.fori_loop(0, n_up, step, 0)

    def dn_phase(src, nxt, base, compute, comm):
        def step(j, carry):
            slot = lax.rem(base + j, RING)
            dn_copy(src, j, slot).wait()
            compute(j, slot)

            @pl.when(j + RING < n_dn)
            def _():
                dn_copy(src, j + RING, slot).start()
            if nxt is not None:
                @pl.when(j + RING >= n_dn)
                def _():
                    dn_copy(nxt, j + RING - n_dn, slot).start()
            comm(j)
            return carry
        lax.fori_loop(0, n_dn, step, 0)

    def down_dot(act_ref, slot):
        total = None
        for i in range(n_up):
            start = min(i * COLS, last_up)
            piece = jnp.dot(act_ref[i], dn_buf[slot, start:start + COLS, :], preferred_element_type=jnp.float32)
            total = piece if total is None else total + piece
        return total

    def put_part(j, first, total):
        half = lax.rem(j, 2)
        for q in range(512 // WIRE):
            for r in range(cuts):
                part[half, first + ((j // 2) * (512 // WIRE) + q) * cuts + r] = total[r * WIRE_ROWS:(r + 1) * WIRE_ROWS, q * WIRE:(q + 1) * WIRE]

    def put_dec(ar, j, total):
        half = lax.rem(j, 2)
        part_d[ar, half, :, pl.ds(pl.multiple_of((j // 2) * 512, 512), 512)] = total

    def no_comm(i):
        pass

    def norm_rows(first):
        blocks = per // cuts
        for r in range(cuts):
            def load(q, r=r):
                return hid[q // blocks, first + lax.rem(q, blocks) * cuts + r].astype(jnp.float32)

            def square(q, acc, load=load):
                val = load(q)
                return acc + val * val
            acc = lax.fori_loop(0, 2 * blocks, square, jnp.zeros((WIRE_ROWS, WIRE), jnp.float32))
            inv = lax.rsqrt(jnp.sum(acc, axis=-1, keepdims=True) / width + NORM_EPS)

            def scale(q, carry, load=load, inv=inv, r=r):
                cols = pl.ds(pl.multiple_of(q * WIRE, WIRE), WIRE)
                normed[r * WIRE_ROWS:(r + 1) * WIRE_ROWS, cols] = (load(q) * inv * norm_a_ref[:, cols].astype(jnp.float32)).astype(jnp.bfloat16)
                return carry
            lax.fori_loop(0, 2 * blocks, scale, 0)

    side = lax.axis_index('side')
    n_side = lax.axis_size('side')
    there = lax.rem(side + n_side // 2, n_side)

    def hand_copy(which, step):
        dest = lax.rem(z + step, 4)
        src, dst = ((keys, k_out), (vals, v_out))[which]
        fold = src.shape[2]
        return pltpu.make_async_remote_copy(
            src_ref=src.at[dest], dst_ref=dst.at[:, pl.ds(pl.multiple_of(z * fold, fold), fold)],
            send_sem=hand_send.at[which, step], recv_sem=hand_recv.at[which, step],
            device_id={'tp': dest, 'side': there}, device_id_type=MESH_ID)

    barrier = pltpu.get_barrier_semaphore()
    for step in range(4):
        pl.semaphore_signal(barrier, inc=1, device_id={'tp': lax.rem(z + step, 4), 'side': there}, device_id_type=MESH_ID)
    for step in (-1, 1):
        @pl.when((z + step >= 0) & (z + step <= 3))
        def _():
            pl.semaphore_signal(barrier, inc=1, device_id={'tp': lax.rem(z + 4 + step, 4)}, device_id_type=MESH_ID)

    for slot in range(RING):
        dn_copy(wo_a, slot, slot).start()
    for slot in range(RING):
        ug_copy(wug_a, slot, slot).start()

    pl.semaphore_wait(barrier, jnp.where((z == 0) | (z == 3), 5, 6))

    depth = 6 * SKEW
    dec_one = per
    dec_two = per + RATE * (n_up + n_dn)
    hand_at = per + depth + 1
    flow_one = (0, 2 * per, False, dec_one)
    flow_c0 = (2 * per, 3 * per, True, dec_two)
    flow_c1 = (2 * per, 4 * per, True, dec_two)

    def slots(first, last, flow):
        def at(s, carry):
            slot_step(s, *flow)
            return carry
        lax.fori_loop(first, last, at, 0)

    def beside(first, last, flow, rate):
        def at(i):
            def one(s, carry):
                slot_step(s, *flow)
                return carry
            lax.fori_loop(jnp.minimum(first + i * rate, last), jnp.minimum(first + (i + 1) * rate, last), one, 0)
        return at

    def prompt_proj(j, slot):
        total = jnp.dot(attn_a_ref[...], dn_buf[slot, :attn_a_ref.shape[1], :], preferred_element_type=jnp.float32)
        put_part(j, 0, total[:HALF_ROWS])
        put_part(j, per, total[HALF_ROWS:])
    dn_phase(wo_a, wo_b, 0, prompt_proj, no_comm)

    def dec_proj(j, slot):
        put_dec(0, j, jnp.dot(attn_b_ref[...], dn_buf[slot, :attn_b_ref.shape[1], :], preferred_element_type=jnp.float32))
    dn_phase(wo_b, wd_a, n_dn, dec_proj, beside(0, n_dn, flow_one, 1))
    slots(n_dn, per + depth, flow_one)

    norm_rows(0)
    ready, drained = per + depth, 2 * per + depth
    lead = min(RATE * n_up, drained - ready)
    up_phase(wug_a, wug_a, 0, normed, act, beside(ready, ready + lead, flow_one, RATE))
    dn_phase(wd_a, wd_a, 2 * n_dn, lambda j, slot: put_part(j, 2 * per, down_dot(act, slot)), beside(ready + lead, drained, flow_one, -(-(drained - ready - lead) // n_dn)))

    norm_rows(per)
    lead = min(RATE * n_up, per)
    up_phase(wug_a, wug_b, n_up, normed, act, beside(0, lead, flow_c0, RATE))
    dn_phase(wd_a, wd_b, 3 * n_dn, lambda j, slot: put_part(j, 3 * per, down_dot(act, slot)), beside(lead, per, flow_c0, -(-(per - lead) // n_dn)))

    val = jnp.concatenate([hid_d[0, 0], hid_d[0, 1]], axis=-1).astype(jnp.float32)
    inv = lax.rsqrt(jnp.mean(val * val, axis=-1, keepdims=True) + NORM_EPS)
    normed_d[...] = (val * inv * norm_b_ref[...].astype(jnp.float32)).astype(jnp.bfloat16)
    up_phase(wug_b, None, 2 * n_up, normed_d, act_d, beside(per, per + RATE * n_up, flow_c1, RATE))
    dn_phase(wd_b, None, 4 * n_dn, lambda j, slot: put_dec(1, j, down_dot(act_d, slot)), beside(per + RATE * n_up, dec_two, flow_c1, RATE))
    slots(dec_two, max(2 * per, dec_two + 1) + depth, flow_c1)

    for which in range(2):
        for step in range(4):
            hand_copy(which, step).wait()
    out_b[:, :mid] = hid_d[1, 0]
    out_b[:, mid:] = hid_d[1, 1]

    for half in range(2):
        for ar in range(2):
            @pl.when(pos(half) < 3)
            def _():
                rsd_copy(ar, half).wait_send()

            @pl.when(pos(half) > 0)
            def _():
                agd_copy(ar, half).wait_send()

    for half in range(2):
        @pl.when(pos(half) < 3)
        def _():
            remote(part.at[half], rcv.at[half], rs_send.at[half], rs_recv.at[half, 0], fwd(half)).wait_send()

        @pl.when(pos(half) > 0)
        def _():
            remote(hid.at[half], hid.at[half], ag_send.at[half], ag_recv.at[half, 0], bwd(half)).wait_send()
        pltpu.make_async_copy(hid.at[half, pl.ds(0, 2 * per)], hid.at[half, pl.ds(2 * per, 2 * per)], out_sem.at[half]).wait()


def block_call(x_rows, y_rows, attn_a, attn_b, norm_a, norm_b, wo_a, wug_a, wd_a, wo_b, wug_b, wd_b, keys, vals):
    rows, width = x_rows.shape
    dec_rows = y_rows.shape[0]
    ffn = wd_a.shape[0]
    mid = width // 2
    cuts = HALF_ROWS // WIRE_ROWS
    per = mid // WIRE * cuts
    n_up = -(-ffn // COLS)
    vmem = pl.BlockSpec(memory_space=pltpu.VMEM)
    hbm = pl.BlockSpec(memory_space=pl.ANY)
    dma = pltpu.SemaphoreType.DMA
    weights = 2 * (wo_a.size + wug_a.size + wd_a.size)
    return pl.pallas_call(
        block_kernel,
        out_shape=(jax.ShapeDtypeStruct((rows, width), jnp.bfloat16), jax.ShapeDtypeStruct((dec_rows, width), jnp.bfloat16),
                   *[jax.ShapeDtypeStruct((rows, keys.shape[0] * keys.shape[2]), jnp.bfloat16)] * 2),
        in_specs=[vmem] * 6 + [hbm] * 8,
        out_specs=(hbm, vmem, hbm, hbm),
        scratch_shapes=[
            pltpu.VMEM((2, 4 * per, WIRE_ROWS, WIRE), jnp.float32),
            pltpu.VMEM((2, 4 * per, WIRE_ROWS, WIRE), jnp.float32),
            pltpu.VMEM((2, 4 * per, WIRE_ROWS, WIRE), jnp.bfloat16),
            pltpu.VMEM((2, 2, dec_rows, mid), jnp.float32),
            pltpu.VMEM((2, 2, dec_rows, mid), jnp.float32),
            pltpu.VMEM((2, 2, dec_rows, mid), jnp.bfloat16),
            pltpu.VMEM((HALF_ROWS, width), jnp.bfloat16),
            pltpu.VMEM((n_up, HALF_ROWS, COLS), jnp.bfloat16),
            pltpu.VMEM((dec_rows, width), jnp.bfloat16),
            pltpu.VMEM((n_up, dec_rows, COLS), jnp.bfloat16),
            pltpu.VMEM((RING, 2, COLS, width), jnp.bfloat16),
            pltpu.VMEM((RING, ffn, 512), jnp.bfloat16),
            dma((2,)), dma((2, 4 * per)), dma((2,)), dma((2, 4 * per)),
            dma((2, 2)), dma((2, 2)), dma((2, 2)), dma((2, 2)),
            dma((RING,)), dma((RING,)), dma((2,)), dma((2, 4)), dma((2, 4)),
        ],
        compiler_params=pltpu.CompilerParams(collective_id=0, has_side_effects=True, vmem_limit_bytes=62 * 1024 * 1024),
        cost_estimate=pl.CostEstimate(flops=weights * (rows + dec_rows) // 2, bytes_accessed=weights * 3, transcendentals=0),
        name='block',
    )(x_rows, y_rows, attn_a, attn_b, norm_a, norm_b, wo_a, wug_a, wd_a, wo_b, wug_b, wd_b, keys, vals)


def front_kernel(s_len, c_len, qkv_a, cos_a, sin_a, slices_b, cos_b, sin_b, wqkv_b, k_cache, v_cache,
                 attn_a, keys, vals, attn_b, k_new, v_new,
                 k_buf, v_buf, w_buf, spread, acc, rows_b, k_in, v_in, k_sem, v_sem, w_sem):
    heads, rows, _ = qkv_a.shape
    head_dim = cos_a.shape[1]
    half = head_dim // 2
    dec_rows, slots_heads, _ = k_cache.shape
    n_tp = keys.shape[0]
    depth = w_buf.shape[1]
    n_w = wqkv_b.shape[0] // depth
    scale = head_dim ** -0.5

    def w_copy(i, slot):
        return pltpu.make_async_copy(wqkv_b.at[pl.ds(pl.multiple_of(i * depth, depth), depth), :], w_buf.at[slot], w_sem.at[slot])

    for slot in range(FRONT_RING):
        w_copy(slot, slot).start()

    def cache_in(b, carry):
        pltpu.make_async_copy(k_cache.at[b], k_buf.at[b], k_in.at[b]).start()
        pltpu.make_async_copy(v_cache.at[b], v_buf.at[b], v_in.at[b]).start()
        return carry
    lax.fori_loop(0, dec_rows, cache_in, 0)

    def rotate(val, cos_tab, sin_tab):
        val = val.astype(jnp.float32)
        swapped = jnp.concatenate([val[:, half:], val[:, :half]], axis=-1)
        return (val * cos_tab + swapped * sin_tab).astype(jnp.bfloat16)

    row = lax.broadcasted_iota(jnp.int32, (rows, rows), 0)
    col = lax.broadcasted_iota(jnp.int32, (rows, rows), 1)
    allowed = (col <= row) & (col < s_len[0])
    valid = lax.broadcasted_iota(jnp.int32, (rows, head_dim), 0) < s_len[0]
    zero = jnp.zeros((rows, head_dim), jnp.float32)
    dims = (((1,), (1,)), ((), ()))
    for h in range(heads):
        query = rotate(qkv_a[h, :, :head_dim], cos_a[...], sin_a[...])
        key = rotate(qkv_a[h, :, head_dim:2 * head_dim], cos_a[...], sin_a[...])
        val = qkv_a[h, :, 2 * head_dim:]
        place = pl.ds((h // n_tp) * head_dim, head_dim)
        keys[h % n_tp, :, place] = jnp.where(valid, key.astype(jnp.float32), zero).astype(jnp.bfloat16)
        vals[h % n_tp, :, place] = jnp.where(valid, val.astype(jnp.float32), zero).astype(jnp.bfloat16)
        scores = lax.dot_general(query, key, dims, preferred_element_type=jnp.float32) * scale
        scores = jnp.where(allowed, scores, -1e30)
        expd = jnp.exp(scores - jnp.max(scores, axis=-1, keepdims=True))
        prob = (expd / jnp.sum(expd, axis=-1, keepdims=True)).astype(jnp.bfloat16)
        attn_a[:, h * head_dim:(h + 1) * head_dim] = jnp.dot(prob, val, preferred_element_type=jnp.float32).astype(jnp.bfloat16)

    lanes = spread.shape[1]
    span = lanes // heads
    one = (lax.broadcasted_iota(jnp.int32, (span, lanes), 1) // heads == lax.broadcasted_iota(jnp.int32, (span, lanes), 0))
    spread[...] = jnp.dot(slices_b[...], jnp.where(one, 1.0, 0.0).astype(jnp.bfloat16), preferred_element_type=jnp.float32)
    own = lax.broadcasted_iota(jnp.int32, (dec_rows, heads, lanes), 2) % heads == lax.broadcasted_iota(jnp.int32, (dec_rows, heads, lanes), 1)
    acc[...] = jnp.zeros_like(acc)
    inner = depth // lanes

    def project(i, carry):
        slot = lax.rem(i, FRONT_RING)
        w_copy(i, slot).wait()
        total = acc[...]
        for j in range(inner):
            part = spread[pl.ds(pl.multiple_of((i * inner + j) * dec_rows, dec_rows), dec_rows), :]
            wide = jnp.where(own, jnp.broadcast_to(part[:, None, :], own.shape), 0.0).reshape(dec_rows * heads, lanes)
            total = total + jnp.dot(wide.astype(jnp.bfloat16), w_buf[slot, j * lanes:(j + 1) * lanes, :], preferred_element_type=jnp.float32)
        acc[...] = total

        @pl.when(i + FRONT_RING < n_w)
        def _():
            w_copy(i + FRONT_RING, slot).start()
        return carry
    lax.fori_loop(0, n_w, project, 0)

    proj = acc[...].astype(jnp.bfloat16)
    rows_b[0] = rotate(proj[:, :head_dim], cos_b[...], sin_b[...]).astype(jnp.float32)
    rows_b[1] = rotate(proj[:, head_dim:2 * head_dim], cos_b[...], sin_b[...]).astype(jnp.float32)
    rows_b[2] = proj[:, 2 * head_dim:].astype(jnp.float32)

    slot_of = lax.broadcasted_iota(jnp.int32, (slots_heads, head_dim), 0) // heads
    pair = lax.broadcasted_iota(jnp.int32, (heads, slots_heads), 1)
    same = pair % heads == lax.broadcasted_iota(jnp.int32, (heads, slots_heads), 0)

    def attend(b, carry):
        length = c_len[b]
        mine = pl.ds(pl.multiple_of(b * heads, heads), heads)

        def updated(buf, new):
            wide = jnp.broadcast_to(new[None], (slots_heads // heads, heads, head_dim)).reshape(slots_heads, head_dim)
            return jnp.where(slot_of == length, wide, buf[b].astype(jnp.float32)).astype(jnp.bfloat16)
        pltpu.make_async_copy(k_cache.at[b], k_buf.at[b], k_in.at[b]).wait()
        k_buf[b] = updated(k_buf, rows_b[1, mine])
        pltpu.make_async_copy(v_cache.at[b], v_buf.at[b], v_in.at[b]).wait()
        v_buf[b] = updated(v_buf, rows_b[2, mine])
        pltpu.make_async_copy(k_buf.at[b], k_new.at[b], k_sem.at[b]).start()
        pltpu.make_async_copy(v_buf.at[b], v_new.at[b], v_sem.at[b]).start()
        scores = lax.dot_general(rows_b[0, mine].astype(jnp.bfloat16), k_buf[b], dims, preferred_element_type=jnp.float32) * scale
        scores = jnp.where(same & (pair // heads <= length), scores, -1e30)
        expd = jnp.exp(scores - jnp.max(scores, axis=-1, keepdims=True))
        prob = (expd / jnp.sum(expd, axis=-1, keepdims=True)).astype(jnp.bfloat16)
        attn_b[b] = jnp.dot(prob, v_buf[b], preferred_element_type=jnp.float32).astype(jnp.bfloat16)
        return carry
    lax.fori_loop(0, dec_rows, attend, 0)

    def cache_out(b, carry):
        pltpu.make_async_copy(k_buf.at[b], k_new.at[b], k_sem.at[b]).wait()
        pltpu.make_async_copy(v_buf.at[b], v_new.at[b], v_sem.at[b]).wait()
        return carry
    lax.fori_loop(0, dec_rows, cache_out, 0)


def rope_tables(positions, head_dim):
    half_dim = head_dim // 2
    inv_freq = ROPE_BASE ** (-jnp.arange(half_dim, dtype=jnp.float32) / half_dim)
    angles = positions.astype(jnp.float32)[:, None] * inv_freq[None, :]
    cos_tab, sin_tab = jnp.cos(angles), jnp.sin(angles)
    return jnp.concatenate([cos_tab, cos_tab], axis=-1), jnp.concatenate([-sin_tab, sin_tab], axis=-1)


def front_call(x_rows, y_rows, s_len, c_len, w_qkv_a, w_qkv_b, gain_a, gain_b, k_cache, v_cache, tp_size):
    num_rows, width = x_rows.shape
    dec_rows = y_rows.shape[0]
    heads, wide = w_qkv_a.shape[1:]
    head_dim = k_cache.shape[-1]
    cache_rows = k_cache.shape[1] * heads
    qkv_a = jnp.einsum('sd,dhe->she', rms_norm(x_rows, gain_a), w_qkv_a, preferred_element_type=jnp.float32).astype(jnp.bfloat16)
    qkv_a = jnp.transpose(qkv_a, (1, 0, 2))
    lanes = 256
    span = lanes // heads
    slices_b = jnp.transpose(rms_norm(y_rows, gain_b).reshape(dec_rows, width // span, span), (1, 0, 2)).reshape(-1, span)
    cos_a, sin_a = rope_tables(jnp.arange(num_rows), head_dim)
    cos_b, sin_b = (jnp.repeat(tab, heads, axis=0) for tab in rope_tables(c_len, head_dim))
    vmem = pl.BlockSpec(memory_space=pltpu.VMEM)
    smem = pl.BlockSpec(memory_space=pltpu.SMEM)
    hbm = pl.BlockSpec(memory_space=pl.ANY)
    dma = pltpu.SemaphoreType.DMA
    depth = 2048
    fold = heads // tp_size * head_dim
    bf16 = jnp.bfloat16
    cache = jax.ShapeDtypeStruct((dec_rows, cache_rows, head_dim), bf16)
    moved = jax.ShapeDtypeStruct((tp_size, num_rows, fold), bf16)
    return pl.pallas_call(
        front_kernel,
        out_shape=(jax.ShapeDtypeStruct((num_rows, heads * head_dim), bf16), moved, moved,
                   jax.ShapeDtypeStruct((dec_rows, heads, head_dim), bf16), cache, cache),
        in_specs=[smem] * 2 + [vmem] * 6 + [hbm] * 3,
        out_specs=(vmem, vmem, vmem, vmem, hbm, hbm),
        scratch_shapes=[
            pltpu.VMEM((dec_rows, cache_rows, head_dim), bf16),
            pltpu.VMEM((dec_rows, cache_rows, head_dim), bf16),
            pltpu.VMEM((FRONT_RING, depth, wide), bf16),
            pltpu.VMEM((width // span * dec_rows, lanes), jnp.float32),
            pltpu.VMEM((dec_rows * heads, wide), jnp.float32),
            pltpu.VMEM((3, dec_rows * heads, head_dim), jnp.float32),
            dma((dec_rows,)), dma((dec_rows,)), dma((dec_rows,)), dma((dec_rows,)), dma((FRONT_RING,)),
        ],
        compiler_params=pltpu.CompilerParams(vmem_limit_bytes=62 * 1024 * 1024),
        cost_estimate=pl.CostEstimate(flops=2 * width * heads * wide * dec_rows, bytes_accessed=60000000, transcendentals=0),
        name='front',
    )(s_len, c_len, qkv_a, cos_a, sin_a, slices_b, cos_b, sin_b, w_qkv_b.reshape(width * heads, wide),
      k_cache.reshape(dec_rows, cache_rows, head_dim), v_cache.reshape(dec_rows, cache_rows, head_dim))


def solution(mesh):
    tp_size = mesh.shape['tp']
    side_size = mesh.shape['side']
    rows_spec = P(('pair', 'side'), None)
    flat_spec = P(('pair', 'side'))
    cache_spec = P(None, ('pair', 'side'), None, None, 'tp', None)
    prompt_spec = P(None, ('pair', 'side'), None, 'tp', None)
    in_specs = (rows_spec, flat_spec, rows_spec, cache_spec, cache_spec, flat_spec,
                P(None, None, 'tp', None), P(None, 'tp', None, None), P(None, None, None, 'tp'), P(None, 'tp', None), P(),
                P(None, None, None, 'tp', None), P(None, None, 'tp', None, None), P(None, None, None, 'tp'), P(None, 'tp', None), P())
    out_specs = (rows_spec, rows_spec, prompt_spec, prompt_spec, cache_spec, cache_spec)

    def body(x_prompt, s_len, y_tok, k_cache, v_cache, c_len, wqkv_a, wo_a, wug_a, wd_a, norm_a, wqkv_b, wo_b, wug_b, wd_b, norm_b):
        width = x_prompt.shape[1]
        head_dim = k_cache.shape[-1]
        dec_rows, slots, heads = k_cache.shape[1:4]
        attn_a, keys, vals, attn_b, k_new, v_new = front_call(
            x_prompt, y_tok, s_len, c_len, wqkv_a[0], wqkv_b[0, :, :, 0], norm_a[0, 0], norm_b[0, 0],
            k_cache[0, :, :, :, 0], v_cache[0, :, :, :, 0], tp_size)
        hidden, y_out, k_prompt, v_prompt = block_call(
            x_prompt, y_tok, attn_a, attn_b.reshape(dec_rows, -1), norm_a[0, 1:2], norm_b[0, 1:2],
            wo_a[0].reshape(-1, width), jnp.transpose(wug_a[0], (1, 2, 0)), wd_a[0],
            wo_b[0].reshape(-1, width), jnp.transpose(wug_b[0], (1, 2, 0)), wd_b[0], keys, vals)
        prompt_shape = (1, x_prompt.shape[0], heads, 1, head_dim)
        return (hidden, y_out, k_prompt.reshape(prompt_shape), v_prompt.reshape(prompt_shape),
                k_new.reshape(k_cache.shape), v_new.reshape(v_cache.shape))

    return jax.shard_map(body, mesh=mesh, in_specs=in_specs, out_specs=out_specs, check_vma=False)
```

```python
import jax
import jax.numpy as jnp
from jax import lax
from jax.experimental import pallas as pl
from jax.experimental.pallas import tpu as pltpu
from jax.sharding import PartitionSpec as P

ROPE_BASE = 10000.0
NORM_EPS = 1e-5


def rms_norm(hidden, gain):
    val_f32 = hidden.astype(jnp.float32)
    inv_rms = lax.rsqrt(jnp.mean(val_f32 * val_f32, axis=-1, keepdims=True) + NORM_EPS)
    return (val_f32 * inv_rms * gain.astype(jnp.float32)).astype(jnp.bfloat16)


def rope_rot(vals_in, positions):
    half_dim = vals_in.shape[-1] // 2
    inv_freq = ROPE_BASE ** (-jnp.arange(half_dim, dtype=jnp.float32) / half_dim)
    angles = positions.astype(jnp.float32)[:, None] * inv_freq[None, :]
    tab_shape = (angles.shape[0],) + (1,) * (vals_in.ndim - 2) + (half_dim,)
    cos_tab = jnp.cos(angles).reshape(tab_shape)
    sin_tab = jnp.sin(angles).reshape(tab_shape)
    lo_half = vals_in[..., :half_dim].astype(jnp.float32)
    hi_half = vals_in[..., half_dim:].astype(jnp.float32)
    return jnp.concatenate([lo_half * cos_tab - hi_half * sin_tab, hi_half * cos_tab + lo_half * sin_tab], axis=-1).astype(jnp.bfloat16)


MESH_ID = pl.DeviceIdType.MESH
COLS = 256
HALF_ROWS = 128
RING = 3
WIRE = 128
WIRE_ROWS = 128
SKEW = 3
RATE = 1


def block_kernel(c_len, x_ref, y_ref, attn_a_ref, slices_b, cos_b, sin_b, norm_a_ref, norm_b_ref, wo_a, wug_a, wd_a, wo_b, wug_b, wd_b, keys, vals, wqkv_b, k_cache, v_cache,
                 out_a, out_b, k_out, v_out, fresh,
                 part, rcv, hid, part_d, rcv_d, hid_d, normed, act, normed_d, act_d, ug_buf, dn_buf,
                 rs_send, rs_recv, ag_send, ag_recv, rsd_send, rsd_recv, agd_send, agd_recv, ug_sem, dn_sem, out_sem, hand_send, hand_recv,
                 k_buf, v_buf, w_buf, spread, acc, rows_b, attn_rows, k_in, v_in, w_sem):
    ffn, width = wd_a.shape
    mid = width // 2
    cuts = HALF_ROWS // WIRE_ROWS
    per = mid // WIRE * cuts
    n_up = -(-ffn // COLS)
    last_up = ffn - COLS
    n_dn = width // 512
    z = lax.axis_index('tp')

    def pos(half):
        return half * z + (1 - half) * (3 - z)

    def fwd(half):
        return lax.rem(z + 4 + (2 * half - 1), 4)

    def bwd(half):
        return lax.rem(z + 4 - (2 * half - 1), 4)

    def remote(src, dst, ssem, rsem, target):
        return pltpu.make_async_remote_copy(src_ref=src, dst_ref=dst, send_sem=ssem, recv_sem=rsem,
                                            device_id={'tp': target}, device_id_type=MESH_ID)

    def rs_copy(half, g):
        return remote(part.at[half, g], rcv.at[half, g], rs_send.at[half], rs_recv.at[half, g], fwd(half))

    def ag_copy(half, g):
        return remote(hid.at[half, g], hid.at[half, g], ag_send.at[half], ag_recv.at[half, g], bwd(half))

    def rsd_copy(ar, half):
        return remote(part_d.at[ar, half], rcv_d.at[ar, half], rsd_send.at[ar, half], rsd_recv.at[ar, half], fwd(half))

    def agd_copy(ar, half):
        return remote(hid_d.at[ar, half], hid_d.at[ar, half], agd_send.at[ar, half], agd_recv.at[ar, half], bwd(half))

    def place(half, g):
        row = (lax.rem(g // per, 2) * cuts + lax.rem(g, cuts)) * WIRE_ROWS
        col = half * mid + lax.rem(g, per) // cuts * WIRE
        return pl.ds(pl.multiple_of(row, WIRE_ROWS), WIRE_ROWS), pl.ds(pl.multiple_of(col, WIRE), WIRE)

    def out_copy(half, g):
        return pltpu.make_async_copy(hid.at[half, g], out_a.at[place(half, g)], out_sem.at[half])

    def ug_copy(src, i, slot):
        row = pl.multiple_of(jnp.minimum(i * COLS, last_up), 64)
        return pltpu.make_async_copy(src.at[:, pl.ds(row, COLS), :], ug_buf.at[slot], ug_sem.at[slot])

    def dn_copy(src, j, slot):
        col = pl.multiple_of(lax.rem(j, 2) * mid + (j // 2) * 512, 512)
        return pltpu.make_async_copy(src.at[:, pl.ds(col, 512)], dn_buf.at[slot, pl.ds(0, src.shape[0]), :], dn_sem.at[slot])

    def slot_step(s, first, last, second, dec_at):
        ar = 1 if second else 0
        if not second:
            for which in range(2):
                turn = s - hand_at - 8 * which

                @pl.when((turn >= 0) & (turn < 8) & (lax.rem(turn, 2) == 0))
                def _():
                    hand_copy(which, turn // 2).start()

        for half in range(2):
            where_at = pos(half)
            g = first + s - SKEW * where_at
            back = first + s - SKEW * (6 - where_at)
            dec = s - dec_at

            @pl.when((where_at == 0) & (g < last))
            def _():
                rs_copy(half, g).start()

            @pl.when((where_at > 0) & (where_at < 3) & (g >= first) & (g < last))
            def _():
                rs_copy(half, g).wait_recv()
                part[half, g] = part[half, g] + rcv[half, g]
                rs_copy(half, g).start()

            @pl.when((where_at == 3) & (g >= first) & (g < last))
            def _():
                rs_copy(half, g).wait_recv()
                total = (part[half, g] + rcv[half, g]).astype(jnp.bfloat16).astype(jnp.float32)
                if second:
                    base = hid[half, g - 2 * per]
                else:
                    base = x_ref[place(half, g)]
                hid[half, g] = (base.astype(jnp.float32) + total).astype(jnp.bfloat16)
                ag_copy(half, g).start()
                if second:
                    out_copy(half, g).start()

            @pl.when((where_at < 3) & (back >= first) & (back < last))
            def _():
                ag_copy(half, back).wait_recv()

                @pl.when(where_at > 0)
                def _():
                    ag_copy(half, back).start()
                if second:
                    out_copy(half, back).start()

            @pl.when((where_at == 0) & (dec == 0))
            def _():
                rsd_copy(ar, half).start()

            @pl.when((where_at > 0) & (where_at < 3) & (dec == SKEW * where_at))
            def _():
                rsd_copy(ar, half).wait_recv()
                part_d[ar, half] = part_d[ar, half] + rcv_d[ar, half]
                rsd_copy(ar, half).start()

            @pl.when((where_at == 3) & (dec == SKEW * where_at))
            def _():
                rsd_copy(ar, half).wait_recv()
                total = (part_d[ar, half] + rcv_d[ar, half]).astype(jnp.bfloat16).astype(jnp.float32)
                base = hid_d[0, half] if ar else y_ref[:, half * mid:(half + 1) * mid]
                hid_d[ar, half] = (base.astype(jnp.float32) + total).astype(jnp.bfloat16)
                agd_copy(ar, half).start()

            @pl.when((where_at < 3) & (dec == SKEW * (6 - where_at)))
            def _():
                agd_copy(ar, half).wait_recv()

                @pl.when(where_at > 0)
                def _():
                    agd_copy(ar, half).start()

    def up_phase(src, nxt, base, lhs_ref, act_ref, comm):
        def step(i, carry):
            slot = lax.rem(base + i, RING)
            ug_copy(src, i, slot).wait()
            lhs = lhs_ref[...]
            dims = (((1,), (1,)), ((), ()))
            up = lax.dot_general(lhs, ug_buf[slot, 0], dims, preferred_element_type=jnp.float32).astype(jnp.bfloat16).astype(jnp.float32)
            gate = lax.dot_general(lhs, ug_buf[slot, 1], dims, preferred_element_type=jnp.float32).astype(jnp.bfloat16).astype(jnp.float32)
            val = jax.nn.silu(gate) * up
            col = lax.broadcasted_iota(jnp.int32, val.shape, 1) + jnp.minimum(i * COLS, last_up)
            act_ref[i] = jnp.where(col >= i * COLS, val, 0.0).astype(jnp.bfloat16)

            @pl.when(i + RING < n_up)
            def _():
                ug_copy(src, i + RING, slot).start()
            if nxt is not None:
                @pl.when(i + RING >= n_up)
                def _():
                    ug_copy(nxt, i + RING - n_up, slot).start()
            comm(i)
            return carry
        lax.fori_loop(0, n_up, step, 0)

    def dn_phase(src, nxt, base, compute, comm):
        def step(j, carry):
            slot = lax.rem(base + j, RING)
            dn_copy(src, j, slot).wait()
            compute(j, slot)

            @pl.when(j + RING < n_dn)
            def _():
                dn_copy(src, j + RING, slot).start()
            if nxt is not None:
                @pl.when(j + RING >= n_dn)
                def _():
                    dn_copy(nxt, j + RING - n_dn, slot).start()
            comm(j)
            return carry
        lax.fori_loop(0, n_dn, step, 0)

    def down_dot(act_ref, slot):
        total = None
        for i in range(n_up):
            start = min(i * COLS, last_up)
            piece = jnp.dot(act_ref[i], dn_buf[slot, start:start + COLS, :], preferred_element_type=jnp.float32)
            total = piece if total is None else total + piece
        return total

    def put_part(j, first, total):
        half = lax.rem(j, 2)
        for q in range(512 // WIRE):
            for r in range(cuts):
                part[half, first + ((j // 2) * (512 // WIRE) + q) * cuts + r] = total[r * WIRE_ROWS:(r + 1) * WIRE_ROWS, q * WIRE:(q + 1) * WIRE]

    def put_dec(ar, j, total):
        half = lax.rem(j, 2)
        part_d[ar, half, :, pl.ds(pl.multiple_of((j // 2) * 512, 512), 512)] = total

    def no_comm(i):
        pass

    def norm_rows(first):
        blocks = per // cuts
        for r in range(cuts):
            def load(q, r=r):
                return hid[q // blocks, first + lax.rem(q, blocks) * cuts + r].astype(jnp.float32)

            def square(q, acc, load=load):
                val = load(q)
                return acc + val * val
            acc = lax.fori_loop(0, 2 * blocks, square, jnp.zeros((WIRE_ROWS, WIRE), jnp.float32))
            inv = lax.rsqrt(jnp.sum(acc, axis=-1, keepdims=True) / width + NORM_EPS)

            def scale(q, carry, load=load, inv=inv, r=r):
                cols = pl.ds(pl.multiple_of(q * WIRE, WIRE), WIRE)
                normed[r * WIRE_ROWS:(r + 1) * WIRE_ROWS, cols] = (load(q) * inv * norm_a_ref[:, cols].astype(jnp.float32)).astype(jnp.bfloat16)
                return carry
            lax.fori_loop(0, 2 * blocks, scale, 0)

    side = lax.axis_index('side')
    n_side = lax.axis_size('side')
    there = lax.rem(side + n_side // 2, n_side)

    def hand_copy(which, step):
        dest = lax.rem(z + step, 4)
        src, dst = ((keys, k_out), (vals, v_out))[which]
        fold = src.shape[2]
        return pltpu.make_async_remote_copy(
            src_ref=src.at[dest], dst_ref=dst.at[:, pl.ds(pl.multiple_of(z * fold, fold), fold)],
            send_sem=hand_send.at[which, step], recv_sem=hand_recv.at[which, step],
            device_id={'tp': dest, 'side': there}, device_id_type=MESH_ID)

    barrier = pltpu.get_barrier_semaphore()
    for step in range(4):
        pl.semaphore_signal(barrier, inc=1, device_id={'tp': lax.rem(z + step, 4), 'side': there}, device_id_type=MESH_ID)
    for step in (-1, 1):
        @pl.when((z + step >= 0) & (z + step <= 3))
        def _():
            pl.semaphore_signal(barrier, inc=1, device_id={'tp': lax.rem(z + 4 + step, 4)}, device_id_type=MESH_ID)

    for slot in range(RING):
        dn_copy(wo_a, slot, slot).start()
    heads = wqkv_b.shape[0] // width
    head_dim = cos_b.shape[1]
    dec_rows, slots_heads, _ = k_cache.shape
    w_depth = w_buf.shape[1]
    n_w = wqkv_b.shape[0] // w_depth

    def w_copy(i, slot):
        return pltpu.make_async_copy(wqkv_b.at[pl.ds(pl.multiple_of(i * w_depth, w_depth), w_depth), :], w_buf.at[slot], w_sem.at[slot])

    def cache_copies(b):
        slot = lax.rem(b, 2)
        return (pltpu.make_async_copy(k_cache.at[b], k_buf.at[slot], k_in.at[slot]),
                pltpu.make_async_copy(v_cache.at[b], v_buf.at[slot], v_in.at[slot]))

    for slot in range(RING):
        w_copy(slot, slot).start()
    for b in range(2):
        for copy in cache_copies(b):
            copy.start()
    for slot in range(RING):
        ug_copy(wug_a, slot, slot).start()

    pl.semaphore_wait(barrier, jnp.where((z == 0) | (z == 3), 5, 6))

    depth = 6 * SKEW
    dec_one = 2 * per
    dec_two = per + RATE * (n_up + n_dn)
    hand_at = per + depth + 1
    flow_one = (0, 2 * per, False, dec_one)
    flow_c0 = (2 * per, 3 * per, True, dec_two)
    flow_c1 = (2 * per, 4 * per, True, dec_two)

    def slots(first, last, flow):
        def at(s, carry):
            slot_step(s, *flow)
            return carry
        lax.fori_loop(first, last, at, 0)

    def beside(first, last, flow, rate):
        def at(i):
            def one(s, carry):
                slot_step(s, *flow)
                return carry
            lax.fori_loop(jnp.minimum(first + i * rate, last), jnp.minimum(first + (i + 1) * rate, last), one, 0)
        return at

    def prompt_proj(j, slot):
        total = jnp.dot(attn_a_ref[...], dn_buf[slot, :attn_a_ref.shape[1], :], preferred_element_type=jnp.float32)
        put_part(j, 0, total[:HALF_ROWS])
        put_part(j, per, total[HALF_ROWS:])
    dn_phase(wo_a, wo_b, 0, prompt_proj, no_comm)

    lanes = spread.shape[1]
    span = lanes // heads
    one = (lax.broadcasted_iota(jnp.int32, (span, lanes), 1) // heads == lax.broadcasted_iota(jnp.int32, (span, lanes), 0))
    spread[...] = jnp.dot(slices_b[...], jnp.where(one, 1.0, 0.0).astype(jnp.bfloat16), preferred_element_type=jnp.float32)
    acc[...] = jnp.zeros_like(acc)
    inner = w_depth // lanes
    early = beside(0, n_w, flow_one, 1)

    def project(i, carry):
        own = lax.broadcasted_iota(jnp.int32, (dec_rows, heads, lanes), 2) % heads == lax.broadcasted_iota(jnp.int32, (dec_rows, heads, lanes), 1)
        slot = lax.rem(i, RING)
        w_copy(i, slot).wait()
        total = acc[...]
        for j in range(inner):
            piece = spread[pl.ds(pl.multiple_of((i * inner + j) * dec_rows, dec_rows), dec_rows), :]
            wide = jnp.where(own, jnp.broadcast_to(piece[:, None, :], own.shape), 0.0).reshape(dec_rows * heads, lanes)
            total = total + jnp.dot(wide.astype(jnp.bfloat16), w_buf[slot, j * lanes:(j + 1) * lanes, :], preferred_element_type=jnp.float32)
        acc[...] = total

        @pl.when(i + RING < n_w)
        def _():
            w_copy(i + RING, slot).start()
        early(i)
        return carry
    lax.fori_loop(0, n_w, project, 0)

    def rotate(val):
        val = val.astype(jnp.float32)
        swapped = jnp.concatenate([val[:, head_dim // 2:], val[:, :head_dim // 2]], axis=-1)
        return (val * cos_b[...] + swapped * sin_b[...]).astype(jnp.bfloat16).astype(jnp.float32)

    proj = acc[...].astype(jnp.bfloat16)
    rows_b[0] = rotate(proj[:, :head_dim])
    rows_b[1] = rotate(proj[:, head_dim:2 * head_dim])
    rows_b[2] = proj[:, 2 * head_dim:].astype(jnp.float32)
    fresh[0] = rows_b[1]
    fresh[1] = rows_b[2]

    late = beside(n_w, n_w + dec_rows, flow_one, 1)

    def attend(b, carry):
        length = c_len[b]
        slot = lax.rem(b, 2)
        mine = pl.ds(pl.multiple_of(b * heads, heads), heads)
        slot_of = lax.broadcasted_iota(jnp.int32, (slots_heads, head_dim), 0) // heads
        pair = lax.broadcasted_iota(jnp.int32, (heads, slots_heads), 1)
        same = pair % heads == lax.broadcasted_iota(jnp.int32, (heads, slots_heads), 0)

        def updated(buf, new):
            wide = jnp.broadcast_to(new[None], (slots_heads // heads, heads, head_dim)).reshape(slots_heads, head_dim)
            return jnp.where(slot_of == length, wide, buf[slot].astype(jnp.float32)).astype(jnp.bfloat16)
        for copy in cache_copies(b):
            copy.wait()
        scores = lax.dot_general(rows_b[0, mine].astype(jnp.bfloat16), updated(k_buf, rows_b[1, mine]), (((1,), (1,)), ((), ())), preferred_element_type=jnp.float32) * head_dim ** -0.5
        scores = jnp.where(same & (pair // heads <= length), scores, -1e30)
        expd = jnp.exp(scores - jnp.max(scores, axis=-1, keepdims=True))
        prob = (expd / jnp.sum(expd, axis=-1, keepdims=True)).astype(jnp.bfloat16)
        attn_rows[b] = jnp.dot(prob, updated(v_buf, rows_b[2, mine]), preferred_element_type=jnp.float32)

        @pl.when(b + 2 < dec_rows)
        def _():
            for copy in cache_copies(b + 2):
                copy.start()
        late(b)
        return carry
    lax.fori_loop(0, dec_rows, attend, 0)

    attn_b = jnp.concatenate([attn_rows[:, h, :] for h in range(heads)], axis=-1).astype(jnp.bfloat16)

    def dec_proj(j, slot):
        put_dec(0, j, jnp.dot(attn_b, dn_buf[slot, :heads * head_dim, :], preferred_element_type=jnp.float32))
    first = n_w + dec_rows
    dn_phase(wo_b, wd_a, n_dn, dec_proj, beside(first, min(first + n_dn, dec_one), flow_one, 1))
    slots(min(first + n_dn, dec_one), per + depth, flow_one)

    norm_rows(0)
    ready, drained = per + depth, max(2 * per, dec_one + 1) + depth
    lead = min(RATE * n_up, drained - ready)
    up_phase(wug_a, wug_a, 0, normed, act, beside(ready, ready + lead, flow_one, RATE))
    dn_phase(wd_a, wd_a, 2 * n_dn, lambda j, slot: put_part(j, 2 * per, down_dot(act, slot)), beside(ready + lead, drained, flow_one, -(-(drained - ready - lead) // n_dn)))

    norm_rows(per)
    lead = min(RATE * n_up, per)
    up_phase(wug_a, wug_b, n_up, normed, act, beside(0, lead, flow_c0, RATE))
    dn_phase(wd_a, wd_b, 3 * n_dn, lambda j, slot: put_part(j, 3 * per, down_dot(act, slot)), beside(lead, per, flow_c0, -(-(per - lead) // n_dn)))

    val = jnp.concatenate([hid_d[0, 0], hid_d[0, 1]], axis=-1).astype(jnp.float32)
    inv = lax.rsqrt(jnp.mean(val * val, axis=-1, keepdims=True) + NORM_EPS)
    normed_d[...] = (val * inv * norm_b_ref[...].astype(jnp.float32)).astype(jnp.bfloat16)
    up_phase(wug_b, None, 2 * n_up, normed_d, act_d, beside(per, per + RATE * n_up, flow_c1, RATE))
    dn_phase(wd_b, None, 4 * n_dn, lambda j, slot: put_dec(1, j, down_dot(act_d, slot)), beside(per + RATE * n_up, dec_two, flow_c1, RATE))
    slots(dec_two, max(2 * per, dec_two + 1) + depth, flow_c1)

    for which in range(2):
        for step in range(4):
            hand_copy(which, step).wait()
    out_b[:, :mid] = hid_d[1, 0]
    out_b[:, mid:] = hid_d[1, 1]

    for half in range(2):
        for ar in range(2):
            @pl.when(pos(half) < 3)
            def _():
                rsd_copy(ar, half).wait_send()

            @pl.when(pos(half) > 0)
            def _():
                agd_copy(ar, half).wait_send()

    for half in range(2):
        @pl.when(pos(half) < 3)
        def _():
            remote(part.at[half], rcv.at[half], rs_send.at[half], rs_recv.at[half, 0], fwd(half)).wait_send()

        @pl.when(pos(half) > 0)
        def _():
            remote(hid.at[half], hid.at[half], ag_send.at[half], ag_recv.at[half, 0], bwd(half)).wait_send()
        pltpu.make_async_copy(hid.at[half, pl.ds(0, 2 * per)], hid.at[half, pl.ds(2 * per, 2 * per)], out_sem.at[half]).wait()


def block_call(c_len, x_rows, y_rows, attn_a, slices_b, cos_b, sin_b, norm_a, norm_b, wo_a, wug_a, wd_a, wo_b, wug_b, wd_b, keys, vals, wqkv_b, k_cache, v_cache):
    rows, width = x_rows.shape
    dec_rows = y_rows.shape[0]
    ffn = wd_a.shape[0]
    mid = width // 2
    cuts = HALF_ROWS // WIRE_ROWS
    per = mid // WIRE * cuts
    n_up = -(-ffn // COLS)
    vmem = pl.BlockSpec(memory_space=pltpu.VMEM)
    hbm = pl.BlockSpec(memory_space=pl.ANY)
    dma = pltpu.SemaphoreType.DMA
    weights = 2 * (wo_a.size + wug_a.size + wd_a.size)
    return pl.pallas_call(
        block_kernel,
        out_shape=(jax.ShapeDtypeStruct((rows, width), jnp.bfloat16), jax.ShapeDtypeStruct((dec_rows, width), jnp.bfloat16),
                   *[jax.ShapeDtypeStruct((rows, keys.shape[0] * keys.shape[2]), jnp.bfloat16)] * 2,
                   jax.ShapeDtypeStruct((2,) + cos_b.shape, jnp.float32)),
        in_specs=[pl.BlockSpec(memory_space=pltpu.SMEM)] + [vmem] * 8 + [hbm] * 11,
        out_specs=(hbm, vmem, hbm, hbm, vmem),
        scratch_shapes=[
            pltpu.VMEM((2, 4 * per, WIRE_ROWS, WIRE), jnp.float32),
            pltpu.VMEM((2, 4 * per, WIRE_ROWS, WIRE), jnp.float32),
            pltpu.VMEM((2, 4 * per, WIRE_ROWS, WIRE), jnp.bfloat16),
            pltpu.VMEM((2, 2, dec_rows, mid), jnp.float32),
            pltpu.VMEM((2, 2, dec_rows, mid), jnp.float32),
            pltpu.VMEM((2, 2, dec_rows, mid), jnp.bfloat16),
            pltpu.VMEM((HALF_ROWS, width), jnp.bfloat16),
            pltpu.VMEM((n_up, HALF_ROWS, COLS), jnp.bfloat16),
            pltpu.VMEM((dec_rows, width), jnp.bfloat16),
            pltpu.VMEM((n_up, dec_rows, COLS), jnp.bfloat16),
            pltpu.VMEM((RING, 2, COLS, width), jnp.bfloat16),
            pltpu.VMEM((RING, ffn, 512), jnp.bfloat16),
            dma((2,)), dma((2, 4 * per)), dma((2,)), dma((2, 4 * per)),
            dma((2, 2)), dma((2, 2)), dma((2, 2)), dma((2, 2)),
            dma((RING,)), dma((RING,)), dma((2,)), dma((2, 4)), dma((2, 4)),
            pltpu.VMEM((2,) + k_cache.shape[1:], jnp.bfloat16),
            pltpu.VMEM((2,) + k_cache.shape[1:], jnp.bfloat16),
            pltpu.VMEM((RING, 2048, wqkv_b.shape[1]), jnp.bfloat16),
            pltpu.VMEM((slices_b.shape[0], 256), jnp.float32),
            pltpu.VMEM((cos_b.shape[0], wqkv_b.shape[1]), jnp.float32),
            pltpu.VMEM((3,) + cos_b.shape, jnp.float32),
            pltpu.VMEM((dec_rows, cos_b.shape[0] // dec_rows, cos_b.shape[1]), jnp.float32),
            dma((2,)), dma((2,)), dma((RING,)),
        ],
        compiler_params=pltpu.CompilerParams(collective_id=0, has_side_effects=True, vmem_limit_bytes=62 * 1024 * 1024),
        cost_estimate=pl.CostEstimate(flops=weights * (rows + dec_rows) // 2, bytes_accessed=weights * 3, transcendentals=0),
        name='block',
    )(c_len, x_rows, y_rows, attn_a, slices_b, cos_b, sin_b, norm_a, norm_b, wo_a, wug_a, wd_a, wo_b, wug_b, wd_b, keys, vals, wqkv_b, k_cache, v_cache)


def front_kernel(s_len, qkv_a, cos_a, sin_a, k_cache, v_cache, attn_a, keys, vals, k_new, v_new, k_buf, v_buf, k_in, v_in, k_sem, v_sem):
    heads, rows, _ = qkv_a.shape
    head_dim = cos_a.shape[1]
    half = head_dim // 2
    dec_rows = k_cache.shape[0]
    n_tp = keys.shape[0]
    scale = head_dim ** -0.5

    def cache_in(b):
        return (pltpu.make_async_copy(k_cache.at[b], k_buf.at[b], k_in.at[b]), pltpu.make_async_copy(v_cache.at[b], v_buf.at[b], v_in.at[b]))

    def cache_out(b):
        return (pltpu.make_async_copy(k_buf.at[b], k_new.at[b], k_sem.at[b]), pltpu.make_async_copy(v_buf.at[b], v_new.at[b], v_sem.at[b]))

    for b in range(dec_rows):
        for copy in cache_in(b):
            copy.start()

    def rotate(val, cos_tab, sin_tab):
        val = val.astype(jnp.float32)
        swapped = jnp.concatenate([val[:, half:], val[:, :half]], axis=-1)
        return (val * cos_tab + swapped * sin_tab).astype(jnp.bfloat16)

    row = lax.broadcasted_iota(jnp.int32, (rows, rows), 0)
    col = lax.broadcasted_iota(jnp.int32, (rows, rows), 1)
    allowed = (col <= row) & (col < s_len[0])
    valid = lax.broadcasted_iota(jnp.int32, (rows, head_dim), 0) < s_len[0]
    zero = jnp.zeros((rows, head_dim), jnp.float32)
    dims = (((1,), (1,)), ((), ()))
    for h in range(heads):
        query = rotate(qkv_a[h, :, :head_dim], cos_a[...], sin_a[...])
        key = rotate(qkv_a[h, :, head_dim:2 * head_dim], cos_a[...], sin_a[...])
        val = qkv_a[h, :, 2 * head_dim:]
        place = pl.ds((h // n_tp) * head_dim, head_dim)
        keys[h % n_tp, :, place] = jnp.where(valid, key.astype(jnp.float32), zero).astype(jnp.bfloat16)
        vals[h % n_tp, :, place] = jnp.where(valid, val.astype(jnp.float32), zero).astype(jnp.bfloat16)
        scores = lax.dot_general(query, key, dims, preferred_element_type=jnp.float32) * scale
        scores = jnp.where(allowed, scores, -1e30)
        expd = jnp.exp(scores - jnp.max(scores, axis=-1, keepdims=True))
        prob = (expd / jnp.sum(expd, axis=-1, keepdims=True)).astype(jnp.bfloat16)
        attn_a[:, h * head_dim:(h + 1) * head_dim] = jnp.dot(prob, val, preferred_element_type=jnp.float32).astype(jnp.bfloat16)
        for b in range(h * dec_rows // heads, (h + 1) * dec_rows // heads):
            for copy in cache_in(b):
                copy.wait()
            for copy in cache_out(b):
                copy.start()
    for b in range(dec_rows):
        for copy in cache_out(b):
            copy.wait()


def insert_kernel(c_len, fresh, k_old, v_old, k_new, v_new, row_buf, row_sem):
    dec_rows, heads, head_dim = row_buf.shape[1:]
    del k_old, v_old
    for which in range(2):
        for b in range(dec_rows):
            row_buf[which, b] = fresh[which, b * heads:(b + 1) * heads, :].astype(jnp.bfloat16)

    def copies(b):
        place = pl.ds(pl.multiple_of(c_len[b] * heads, heads), heads)
        return [pltpu.make_async_copy(row_buf.at[which, b], dst.at[b, place, :], row_sem.at[which, b]) for which, dst in enumerate((k_new, v_new))]
    for b in range(dec_rows):
        for copy in copies(b):
            copy.start()
    for b in range(dec_rows):
        for copy in copies(b):
            copy.wait()


def insert_call(c_len, fresh, k_copy, v_copy):
    dec_rows = k_copy.shape[0]
    head_dim = k_copy.shape[2]
    heads = fresh.shape[1] // dec_rows
    hbm = pl.BlockSpec(memory_space=pl.ANY)
    return pl.pallas_call(
        insert_kernel,
        out_shape=(jax.ShapeDtypeStruct(k_copy.shape, k_copy.dtype),) * 2,
        in_specs=[pl.BlockSpec(memory_space=pltpu.SMEM), pl.BlockSpec(memory_space=pltpu.VMEM), hbm, hbm],
        out_specs=(hbm, hbm),
        scratch_shapes=[pltpu.VMEM((2, dec_rows, heads, head_dim), jnp.bfloat16), pltpu.SemaphoreType.DMA((2, dec_rows))],
        input_output_aliases={2: 0, 3: 1},
        compiler_params=pltpu.CompilerParams(vmem_limit_bytes=62 * 1024 * 1024),
        name='insert',
    )(c_len, fresh, k_copy, v_copy)


def rope_tables(positions, head_dim):
    half_dim = head_dim // 2
    inv_freq = ROPE_BASE ** (-jnp.arange(half_dim, dtype=jnp.float32) / half_dim)
    angles = positions.astype(jnp.float32)[:, None] * inv_freq[None, :]
    cos_tab, sin_tab = jnp.cos(angles), jnp.sin(angles)
    return jnp.concatenate([cos_tab, cos_tab], axis=-1), jnp.concatenate([-sin_tab, sin_tab], axis=-1)


def decode_operands(y_rows, c_len, gain_b, heads, head_dim):
    dec_rows, width = y_rows.shape
    span = 256 // heads
    slices_b = jnp.transpose(rms_norm(y_rows, gain_b).reshape(dec_rows, width // span, span), (1, 0, 2)).reshape(-1, span)
    cos_b, sin_b = (jnp.repeat(tab, heads, axis=0) for tab in rope_tables(c_len, head_dim))
    return slices_b, cos_b, sin_b


def front_call(x_rows, s_len, w_qkv_a, gain_a, k_cache, v_cache, tp_size):
    num_rows, width = x_rows.shape
    heads, wide = w_qkv_a.shape[1:]
    dec_rows, cache_rows, head_dim = k_cache.shape
    qkv_a = jnp.einsum('sd,dhe->she', rms_norm(x_rows, gain_a), w_qkv_a, preferred_element_type=jnp.float32).astype(jnp.bfloat16)
    qkv_a = jnp.transpose(qkv_a, (1, 0, 2))
    cos_a, sin_a = rope_tables(jnp.arange(num_rows), head_dim)
    vmem = pl.BlockSpec(memory_space=pltpu.VMEM)
    hbm = pl.BlockSpec(memory_space=pl.ANY)
    dma = pltpu.SemaphoreType.DMA
    bf16 = jnp.bfloat16
    cache = jax.ShapeDtypeStruct((dec_rows, cache_rows, head_dim), bf16)
    moved = jax.ShapeDtypeStruct((tp_size, num_rows, heads // tp_size * head_dim), bf16)
    return pl.pallas_call(
        front_kernel,
        out_shape=(jax.ShapeDtypeStruct((num_rows, heads * head_dim), bf16), moved, moved, cache, cache),
        in_specs=[pl.BlockSpec(memory_space=pltpu.SMEM)] + [vmem] * 3 + [hbm] * 2,
        out_specs=(vmem, vmem, vmem, hbm, hbm),
        scratch_shapes=[pltpu.VMEM(cache.shape, bf16)] * 2 + [dma((dec_rows,))] * 4,
        compiler_params=pltpu.CompilerParams(vmem_limit_bytes=62 * 1024 * 1024),
        cost_estimate=pl.CostEstimate(flops=8 * num_rows * num_rows * heads * head_dim, bytes_accessed=8 * k_cache.size, transcendentals=0),
        name='front',
    )(s_len, qkv_a, cos_a, sin_a, k_cache, v_cache)


def solution(mesh):
    tp_size = mesh.shape['tp']
    side_size = mesh.shape['side']
    rows_spec = P(('pair', 'side'), None)
    flat_spec = P(('pair', 'side'))
    cache_spec = P(None, ('pair', 'side'), None, None, 'tp', None)
    prompt_spec = P(None, ('pair', 'side'), None, 'tp', None)
    in_specs = (rows_spec, flat_spec, rows_spec, cache_spec, cache_spec, flat_spec,
                P(None, None, 'tp', None), P(None, 'tp', None, None), P(None, None, None, 'tp'), P(None, 'tp', None), P(),
                P(None, None, None, 'tp', None), P(None, None, 'tp', None, None), P(None, None, None, 'tp'), P(None, 'tp', None), P())
    out_specs = (rows_spec, rows_spec, prompt_spec, prompt_spec, cache_spec, cache_spec)

    def body(x_prompt, s_len, y_tok, k_cache, v_cache, c_len, wqkv_a, wo_a, wug_a, wd_a, norm_a, wqkv_b, wo_b, wug_b, wd_b, norm_b):
        width = x_prompt.shape[1]
        head_dim = k_cache.shape[-1]
        dec_rows, slots, heads = k_cache.shape[1:4]
        k_rows = k_cache.reshape(dec_rows, slots * heads, head_dim)
        v_rows = v_cache.reshape(dec_rows, slots * heads, head_dim)
        attn_a, keys, vals, k_copy, v_copy = front_call(x_prompt, s_len, wqkv_a[0], norm_a[0, 0], k_rows, v_rows, tp_size)
        slices_b, cos_b, sin_b = decode_operands(y_tok, c_len, norm_b[0, 0], heads, head_dim)
        hidden, y_out, k_prompt, v_prompt, fresh = block_call(
            c_len, x_prompt, y_tok, attn_a, slices_b, cos_b, sin_b, norm_a[0, 1:2], norm_b[0, 1:2],
            wo_a[0].reshape(-1, width), jnp.transpose(wug_a[0], (1, 2, 0)), wd_a[0],
            wo_b[0].reshape(-1, width), jnp.transpose(wug_b[0], (1, 2, 0)), wd_b[0], keys, vals,
            wqkv_b.reshape(width * heads, -1), k_rows, v_rows)
        k_new, v_new = insert_call(c_len, fresh, k_copy, v_copy)
        prompt_shape = (1, x_prompt.shape[0], heads, 1, head_dim)
        return (hidden, y_out, k_prompt.reshape(prompt_shape), v_prompt.reshape(prompt_shape),
                k_new.reshape(k_cache.shape), v_new.reshape(v_cache.shape))

    return jax.shard_map(body, mesh=mesh, in_specs=in_specs, out_specs=out_specs, check_vma=False)
```

```python
import jax
import jax.numpy as jnp
import numpy as np
from jax import lax
from jax.experimental import pallas as pl
from jax.experimental.pallas import tpu as pltpu
from jax.sharding import PartitionSpec as P

ROPE_BASE = 10000.0
NORM_EPS = 1e-5


def rms_norm(hidden, gain):
    val_f32 = hidden.astype(jnp.float32)
    inv_rms = lax.rsqrt(jnp.mean(val_f32 * val_f32, axis=-1, keepdims=True) + NORM_EPS)
    return (val_f32 * inv_rms * gain.astype(jnp.float32)).astype(jnp.bfloat16)


def rope_rot(vals_in, positions):
    half_dim = vals_in.shape[-1] // 2
    inv_freq = ROPE_BASE ** (-jnp.arange(half_dim, dtype=jnp.float32) / half_dim)
    angles = positions.astype(jnp.float32)[:, None] * inv_freq[None, :]
    tab_shape = (angles.shape[0],) + (1,) * (vals_in.ndim - 2) + (half_dim,)
    cos_tab = jnp.cos(angles).reshape(tab_shape)
    sin_tab = jnp.sin(angles).reshape(tab_shape)
    lo_half = vals_in[..., :half_dim].astype(jnp.float32)
    hi_half = vals_in[..., half_dim:].astype(jnp.float32)
    return jnp.concatenate([lo_half * cos_tab - hi_half * sin_tab, hi_half * cos_tab + lo_half * sin_tab], axis=-1).astype(jnp.bfloat16)


MESH_ID = pl.DeviceIdType.MESH
COLS = 256
HALF_ROWS = 128
RING = 3
WIRE = 128
WIRE_ROWS = 128
SKEW = 3
RATE = 1


def block_kernel(c_len, x_ref, y_ref, attn_a_ref, cos_tab, sin_tab, norm_a_ref, norm_b_ref, wo_a, wug_a, wd_a, wo_b, wug_b, wd_b, keys, vals, wqkv_b, k_cache, v_cache,
                 out_a, out_b, k_out, v_out, fresh,
                 part, rcv, hid, part_d, rcv_d, hid_d, normed, act, normed_d, act_d, ug_buf, dn_buf,
                 rs_send, rs_recv, ag_send, ag_recv, rsd_send, rsd_recv, agd_send, agd_recv, ug_sem, dn_sem, out_sem, hand_send, hand_recv,
                 k_buf, v_buf, w_buf, spread, acc, rows_b, attn_rows, k_in, v_in, w_sem):
    ffn, width = wd_a.shape
    mid = width // 2
    cuts = HALF_ROWS // WIRE_ROWS
    per = mid // WIRE * cuts
    n_up = -(-ffn // COLS)
    last_up = ffn - COLS
    n_dn = width // 512
    z = lax.axis_index('tp')

    def pos(half):
        return half * z + (1 - half) * (3 - z)

    def fwd(half):
        return lax.rem(z + 4 + (2 * half - 1), 4)

    def bwd(half):
        return lax.rem(z + 4 - (2 * half - 1), 4)

    def remote(src, dst, ssem, rsem, target):
        return pltpu.make_async_remote_copy(src_ref=src, dst_ref=dst, send_sem=ssem, recv_sem=rsem,
                                            device_id={'tp': target}, device_id_type=MESH_ID)

    def rs_copy(half, g):
        return remote(part.at[half, g], rcv.at[half, g], rs_send.at[half], rs_recv.at[half, g], fwd(half))

    def ag_copy(half, g):
        return remote(hid.at[half, g], hid.at[half, g], ag_send.at[half], ag_recv.at[half, g], bwd(half))

    def rsd_copy(ar, half):
        return remote(part_d.at[ar, half], rcv_d.at[ar, half], rsd_send.at[ar, half], rsd_recv.at[ar, half], fwd(half))

    def agd_copy(ar, half):
        return remote(hid_d.at[ar, half], hid_d.at[ar, half], agd_send.at[ar, half], agd_recv.at[ar, half], bwd(half))

    def place(half, g):
        row = (lax.rem(g // per, 2) * cuts + lax.rem(g, cuts)) * WIRE_ROWS
        col = half * mid + lax.rem(g, per) // cuts * WIRE
        return pl.ds(pl.multiple_of(row, WIRE_ROWS), WIRE_ROWS), pl.ds(pl.multiple_of(col, WIRE), WIRE)

    def out_copy(half, g):
        return pltpu.make_async_copy(hid.at[half, g], out_a.at[place(half, g)], out_sem.at[half])

    def ug_copy(src, i, slot):
        row = pl.multiple_of(jnp.minimum(i * COLS, last_up), 64)
        return pltpu.make_async_copy(src.at[:, pl.ds(row, COLS), :], ug_buf.at[slot], ug_sem.at[slot])

    def dn_copy(src, j, slot):
        col = pl.multiple_of(lax.rem(j, 2) * mid + (j // 2) * 512, 512)
        return pltpu.make_async_copy(src.at[:, pl.ds(col, 512)], dn_buf.at[slot, pl.ds(0, src.shape[0]), :], dn_sem.at[slot])

    def slot_step(s, first, last, second, dec_at):
        ar = 1 if second else 0
        if not second:
            for which in range(2):
                turn = s - hand_at - 8 * which

                @pl.when((turn >= 0) & (turn < 8) & (lax.rem(turn, 2) == 0))
                def _():
                    hand_copy(which, turn // 2).start()

        for half in range(2):
            where_at = pos(half)
            g = first + s - SKEW * where_at
            back = first + s - SKEW * (6 - where_at)
            dec = s - dec_at

            @pl.when((where_at == 0) & (g < last))
            def _():
                rs_copy(half, g).start()

            @pl.when((where_at > 0) & (where_at < 3) & (g >= first) & (g < last))
            def _():
                rs_copy(half, g).wait_recv()
                part[half, g] = part[half, g] + rcv[half, g]
                rs_copy(half, g).start()

            @pl.when((where_at == 3) & (g >= first) & (g < last))
            def _():
                rs_copy(half, g).wait_recv()
                total = (part[half, g] + rcv[half, g]).astype(jnp.bfloat16).astype(jnp.float32)
                if second:
                    base = hid[half, g - 2 * per]
                else:
                    base = x_ref[place(half, g)]
                hid[half, g] = (base.astype(jnp.float32) + total).astype(jnp.bfloat16)
                ag_copy(half, g).start()
                if second:
                    out_copy(half, g).start()

            @pl.when((where_at < 3) & (back >= first) & (back < last))
            def _():
                ag_copy(half, back).wait_recv()

                @pl.when(where_at > 0)
                def _():
                    ag_copy(half, back).start()
                if second:
                    out_copy(half, back).start()

            @pl.when((where_at == 0) & (dec == 0))
            def _():
                rsd_copy(ar, half).start()

            @pl.when((where_at > 0) & (where_at < 3) & (dec == SKEW * where_at))
            def _():
                rsd_copy(ar, half).wait_recv()
                part_d[ar, half] = part_d[ar, half] + rcv_d[ar, half]
                rsd_copy(ar, half).start()

            @pl.when((where_at == 3) & (dec == SKEW * where_at))
            def _():
                rsd_copy(ar, half).wait_recv()
                total = (part_d[ar, half] + rcv_d[ar, half]).astype(jnp.bfloat16).astype(jnp.float32)
                base = hid_d[0, half] if ar else y_ref[:, half * mid:(half + 1) * mid]
                hid_d[ar, half] = (base.astype(jnp.float32) + total).astype(jnp.bfloat16)
                agd_copy(ar, half).start()

            @pl.when((where_at < 3) & (dec == SKEW * (6 - where_at)))
            def _():
                agd_copy(ar, half).wait_recv()

                @pl.when(where_at > 0)
                def _():
                    agd_copy(ar, half).start()

    def up_phase(src, nxt, base, lhs_ref, act_ref, comm):
        def step(i, carry):
            slot = lax.rem(base + i, RING)
            ug_copy(src, i, slot).wait()
            lhs = lhs_ref[...]
            dims = (((1,), (1,)), ((), ()))
            up = lax.dot_general(lhs, ug_buf[slot, 0], dims, preferred_element_type=jnp.float32).astype(jnp.bfloat16).astype(jnp.float32)
            gate = lax.dot_general(lhs, ug_buf[slot, 1], dims, preferred_element_type=jnp.float32).astype(jnp.bfloat16).astype(jnp.float32)
            val = jax.nn.silu(gate) * up
            col = lax.broadcasted_iota(jnp.int32, val.shape, 1) + jnp.minimum(i * COLS, last_up)
            act_ref[i] = jnp.where(col >= i * COLS, val, 0.0).astype(jnp.bfloat16)

            @pl.when(i + RING < n_up)
            def _():
                ug_copy(src, i + RING, slot).start()
            if nxt is not None:
                @pl.when(i + RING >= n_up)
                def _():
                    ug_copy(nxt, i + RING - n_up, slot).start()
            comm(i)
            return carry
        lax.fori_loop(0, n_up, step, 0)

    def dn_phase(src, nxt, base, compute, comm):
        def step(j, carry):
            slot = lax.rem(base + j, RING)
            dn_copy(src, j, slot).wait()
            compute(j, slot)

            @pl.when(j + RING < n_dn)
            def _():
                dn_copy(src, j + RING, slot).start()
            if nxt is not None:
                @pl.when(j + RING >= n_dn)
                def _():
                    dn_copy(nxt, j + RING - n_dn, slot).start()
            comm(j)
            return carry
        lax.fori_loop(0, n_dn, step, 0)

    def down_dot(act_ref, slot):
        total = None
        for i in range(n_up):
            start = min(i * COLS, last_up)
            piece = jnp.dot(act_ref[i], dn_buf[slot, start:start + COLS, :], preferred_element_type=jnp.float32)
            total = piece if total is None else total + piece
        return total

    def put_part(j, first, total):
        half = lax.rem(j, 2)
        for q in range(512 // WIRE):
            for r in range(cuts):
                part[half, first + ((j // 2) * (512 // WIRE) + q) * cuts + r] = total[r * WIRE_ROWS:(r + 1) * WIRE_ROWS, q * WIRE:(q + 1) * WIRE]

    def put_dec(ar, j, total):
        half = lax.rem(j, 2)
        part_d[ar, half, :, pl.ds(pl.multiple_of((j // 2) * 512, 512), 512)] = total

    def no_comm(i):
        pass

    def norm_rows(first):
        blocks = per // cuts
        for r in range(cuts):
            def load(q, r=r):
                return hid[q // blocks, first + lax.rem(q, blocks) * cuts + r].astype(jnp.float32)

            def square(q, acc, load=load):
                val = load(q)
                return acc + val * val
            acc = lax.fori_loop(0, 2 * blocks, square, jnp.zeros((WIRE_ROWS, WIRE), jnp.float32))
            inv = lax.rsqrt(jnp.sum(acc, axis=-1, keepdims=True) / width + NORM_EPS)

            def scale(q, carry, load=load, inv=inv, r=r):
                cols = pl.ds(pl.multiple_of(q * WIRE, WIRE), WIRE)
                normed[r * WIRE_ROWS:(r + 1) * WIRE_ROWS, cols] = (load(q) * inv * norm_a_ref[1:2, cols].astype(jnp.float32)).astype(jnp.bfloat16)
                return carry
            lax.fori_loop(0, 2 * blocks, scale, 0)

    side = lax.axis_index('side')
    n_side = lax.axis_size('side')
    there = lax.rem(side + n_side // 2, n_side)

    def hand_copy(which, step):
        dest = lax.rem(z + step, 4)
        src, dst = ((keys, k_out), (vals, v_out))[which]
        fold = src.shape[2]
        return pltpu.make_async_remote_copy(
            src_ref=src.at[dest], dst_ref=dst.at[:, pl.ds(pl.multiple_of(z * fold, fold), fold)],
            send_sem=hand_send.at[which, step], recv_sem=hand_recv.at[which, step],
            device_id={'tp': dest, 'side': there}, device_id_type=MESH_ID)

    barrier = pltpu.get_barrier_semaphore()
    for step in range(4):
        pl.semaphore_signal(barrier, inc=1, device_id={'tp': lax.rem(z + step, 4), 'side': there}, device_id_type=MESH_ID)
    for step in (-1, 1):
        @pl.when((z + step >= 0) & (z + step <= 3))
        def _():
            pl.semaphore_signal(barrier, inc=1, device_id={'tp': lax.rem(z + 4 + step, 4)}, device_id_type=MESH_ID)

    for slot in range(RING):
        dn_copy(wo_a, slot, slot).start()
    heads = wqkv_b.shape[0] // width
    head_dim = cos_tab.shape[1]
    dec_rows, slots_heads, _ = k_cache.shape
    w_depth = w_buf.shape[1]
    n_w = wqkv_b.shape[0] // w_depth

    def w_copy(i, slot):
        return pltpu.make_async_copy(wqkv_b.at[pl.ds(pl.multiple_of(i * w_depth, w_depth), w_depth), :], w_buf.at[slot], w_sem.at[slot])

    def cache_copies(b):
        slot = lax.rem(b, 2)
        return (pltpu.make_async_copy(k_cache.at[b], k_buf.at[slot], k_in.at[slot]),
                pltpu.make_async_copy(v_cache.at[b], v_buf.at[slot], v_in.at[slot]))

    for slot in range(RING):
        w_copy(slot, slot).start()
    for b in range(2):
        for copy in cache_copies(b):
            copy.start()
    for slot in range(RING):
        ug_copy(wug_a, slot, slot).start()

    pl.semaphore_wait(barrier, jnp.where((z == 0) | (z == 3), 5, 6))

    depth = 6 * SKEW
    dec_one = 2 * per
    dec_two = per + RATE * (n_up + n_dn)
    hand_at = per + depth + 1
    flow_one = (0, 2 * per, False, dec_one)
    flow_c0 = (2 * per, 3 * per, True, dec_two)
    flow_c1 = (2 * per, 4 * per, True, dec_two)

    def slots(first, last, flow):
        def at(s, carry):
            slot_step(s, *flow)
            return carry
        lax.fori_loop(first, last, at, 0)

    def beside(first, last, flow, rate):
        def at(i):
            def one(s, carry):
                slot_step(s, *flow)
                return carry
            lax.fori_loop(jnp.minimum(first + i * rate, last), jnp.minimum(first + (i + 1) * rate, last), one, 0)
        return at

    def prompt_proj(j, slot):
        total = jnp.dot(attn_a_ref[...], dn_buf[slot, :attn_a_ref.shape[1], :], preferred_element_type=jnp.float32)
        put_part(j, 0, total[:HALF_ROWS])
        put_part(j, per, total[HALF_ROWS:])
    dn_phase(wo_a, wo_b, 0, prompt_proj, no_comm)

    lanes = spread.shape[1]
    span = lanes // heads
    group = 4
    one = (lax.broadcasted_iota(jnp.int32, (group * span, group * lanes), 1) // heads == lax.broadcasted_iota(jnp.int32, (group * span, group * lanes), 0))
    one = jnp.where(one, 1.0, 0.0).astype(jnp.bfloat16)
    val = y_ref[...].astype(jnp.float32)
    inv = lax.rsqrt(jnp.mean(val * val, axis=-1, keepdims=True) + NORM_EPS)
    normed_d[...] = (val * inv * norm_b_ref[0:1, :].astype(jnp.float32)).astype(jnp.bfloat16)
    n_spread = width // (group * span)
    first_slots = 8

    def widen(i, carry):
        for e in range(n_spread // first_slots):
            at = i * (n_spread // first_slots) + e
            cols = pl.ds(pl.multiple_of(at * group * span, group * span), group * span)
            block = jnp.dot(normed_d[:, cols], one, preferred_element_type=jnp.float32)
            for q in range(group):
                spread[pl.ds(pl.multiple_of((at * group + q) * dec_rows, dec_rows), dec_rows), :] = block[:, q * lanes:(q + 1) * lanes]
        slot_step(i, *flow_one)
        return carry
    lax.fori_loop(0, first_slots, widen, 0)
    acc[...] = jnp.zeros_like(acc)
    inner = w_depth // lanes
    early = beside(first_slots, first_slots + n_w, flow_one, 1)

    def project(i, carry):
        own = lax.broadcasted_iota(jnp.int32, (dec_rows, heads, lanes), 2) % heads == lax.broadcasted_iota(jnp.int32, (dec_rows, heads, lanes), 1)
        slot = lax.rem(i, RING)
        w_copy(i, slot).wait()
        total = acc[...]
        for j in range(inner):
            piece = spread[pl.ds(pl.multiple_of((i * inner + j) * dec_rows, dec_rows), dec_rows), :]
            wide = jnp.where(own, jnp.broadcast_to(piece[:, None, :], own.shape), 0.0).reshape(dec_rows * heads, lanes)
            total = total + jnp.dot(wide.astype(jnp.bfloat16), w_buf[slot, j * lanes:(j + 1) * lanes, :], preferred_element_type=jnp.float32)
        acc[...] = total

        @pl.when(i + RING < n_w)
        def _():
            w_copy(i + RING, slot).start()
        early(i)
        return carry
    lax.fori_loop(0, n_w, project, 0)

    def rotate(val):
        val = val.astype(jnp.float32)
        swapped = jnp.concatenate([val[:, head_dim // 2:], val[:, :head_dim // 2]], axis=-1)
        return (val * cos_b + swapped * sin_b).astype(jnp.bfloat16).astype(jnp.float32)

    def by_row(tab):
        return jnp.concatenate([jnp.broadcast_to(tab[pl.ds(c_len[b], 1), :], (heads, head_dim)) for b in range(dec_rows)], axis=0)
    cos_b, sin_b = by_row(cos_tab), by_row(sin_tab)
    proj = acc[...].astype(jnp.bfloat16)
    rows_b[0] = rotate(proj[:, :head_dim])
    rows_b[1] = rotate(proj[:, head_dim:2 * head_dim])
    rows_b[2] = proj[:, 2 * head_dim:].astype(jnp.float32)
    fresh[0] = rows_b[1]
    fresh[1] = rows_b[2]

    late = beside(first_slots + n_w, first_slots + n_w + dec_rows, flow_one, 1)

    def attend(b, carry):
        length = c_len[b]
        slot = lax.rem(b, 2)
        mine = pl.ds(pl.multiple_of(b * heads, heads), heads)
        slot_of = lax.broadcasted_iota(jnp.int32, (slots_heads, head_dim), 0) // heads
        pair = lax.broadcasted_iota(jnp.int32, (heads, slots_heads), 1)
        same = pair % heads == lax.broadcasted_iota(jnp.int32, (heads, slots_heads), 0)

        def updated(buf, new):
            wide = jnp.broadcast_to(new[None], (slots_heads // heads, heads, head_dim)).reshape(slots_heads, head_dim)
            return jnp.where(slot_of == length, wide, buf[slot].astype(jnp.float32)).astype(jnp.bfloat16)
        for copy in cache_copies(b):
            copy.wait()
        scores = lax.dot_general(rows_b[0, mine].astype(jnp.bfloat16), updated(k_buf, rows_b[1, mine]), (((1,), (1,)), ((), ())), preferred_element_type=jnp.float32) * head_dim ** -0.5
        scores = jnp.where(same & (pair // heads <= length), scores, -1e30)
        expd = jnp.exp(scores - jnp.max(scores, axis=-1, keepdims=True))
        prob = (expd / jnp.sum(expd, axis=-1, keepdims=True)).astype(jnp.bfloat16)
        attn_rows[b] = jnp.dot(prob, updated(v_buf, rows_b[2, mine]), preferred_element_type=jnp.float32)

        @pl.when(b + 2 < dec_rows)
        def _():
            for copy in cache_copies(b + 2):
                copy.start()
        late(b)
        return carry
    lax.fori_loop(0, dec_rows, attend, 0)

    attn_b = jnp.concatenate([attn_rows[:, h, :] for h in range(heads)], axis=-1).astype(jnp.bfloat16)

    def dec_proj(j, slot):
        put_dec(0, j, jnp.dot(attn_b, dn_buf[slot, :heads * head_dim, :], preferred_element_type=jnp.float32))
    first = first_slots + n_w + dec_rows
    dn_phase(wo_b, wd_a, n_dn, dec_proj, beside(first, min(first + n_dn, dec_one), flow_one, 1))
    slots(min(first + n_dn, dec_one), per + depth, flow_one)

    norm_rows(0)
    ready, drained = per + depth, max(2 * per, dec_one + 1) + depth
    lead = min(RATE * n_up, drained - ready)
    up_phase(wug_a, wug_a, 0, normed, act, beside(ready, ready + lead, flow_one, RATE))
    dn_phase(wd_a, wd_a, 2 * n_dn, lambda j, slot: put_part(j, 2 * per, down_dot(act, slot)), beside(ready + lead, drained, flow_one, -(-(drained - ready - lead) // n_dn)))

    norm_rows(per)
    lead = min(RATE * n_up, per)
    up_phase(wug_a, wug_b, n_up, normed, act, beside(0, lead, flow_c0, RATE))
    dn_phase(wd_a, wd_b, 3 * n_dn, lambda j, slot: put_part(j, 3 * per, down_dot(act, slot)), beside(lead, per, flow_c0, -(-(per - lead) // n_dn)))

    val = jnp.concatenate([hid_d[0, 0], hid_d[0, 1]], axis=-1).astype(jnp.float32)
    inv = lax.rsqrt(jnp.mean(val * val, axis=-1, keepdims=True) + NORM_EPS)
    normed_d[...] = (val * inv * norm_b_ref[1:2, :].astype(jnp.float32)).astype(jnp.bfloat16)
    up_phase(wug_b, None, 2 * n_up, normed_d, act_d, beside(per, per + RATE * n_up, flow_c1, RATE))
    dn_phase(wd_b, None, 4 * n_dn, lambda j, slot: put_dec(1, j, down_dot(act_d, slot)), beside(per + RATE * n_up, dec_two, flow_c1, RATE))
    slots(dec_two, max(2 * per, dec_two + 1) + depth, flow_c1)

    for which in range(2):
        for step in range(4):
            hand_copy(which, step).wait()
    out_b[:, :mid] = hid_d[1, 0]
    out_b[:, mid:] = hid_d[1, 1]

    for half in range(2):
        for ar in range(2):
            @pl.when(pos(half) < 3)
            def _():
                rsd_copy(ar, half).wait_send()

            @pl.when(pos(half) > 0)
            def _():
                agd_copy(ar, half).wait_send()

    for half in range(2):
        @pl.when(pos(half) < 3)
        def _():
            remote(part.at[half], rcv.at[half], rs_send.at[half], rs_recv.at[half, 0], fwd(half)).wait_send()

        @pl.when(pos(half) > 0)
        def _():
            remote(hid.at[half], hid.at[half], ag_send.at[half], ag_recv.at[half, 0], bwd(half)).wait_send()
        pltpu.make_async_copy(hid.at[half, pl.ds(0, 2 * per)], hid.at[half, pl.ds(2 * per, 2 * per)], out_sem.at[half]).wait()


def block_call(c_len, x_rows, y_rows, attn_a, cos_tab, sin_tab, norm_a, norm_b, wo_a, wug_a, wd_a, wo_b, wug_b, wd_b, keys, vals, wqkv_b, k_cache, v_cache):
    rows, width = x_rows.shape
    dec_rows = y_rows.shape[0]
    heads, head_dim = wqkv_b.shape[0] // width, cos_tab.shape[1]
    ffn = wd_a.shape[0]
    mid = width // 2
    cuts = HALF_ROWS // WIRE_ROWS
    per = mid // WIRE * cuts
    n_up = -(-ffn // COLS)
    vmem = pl.BlockSpec(memory_space=pltpu.VMEM)
    hbm = pl.BlockSpec(memory_space=pl.ANY)
    dma = pltpu.SemaphoreType.DMA
    weights = 2 * (wo_a.size + wug_a.size + wd_a.size)
    return pl.pallas_call(
        block_kernel,
        out_shape=(jax.ShapeDtypeStruct((rows, width), jnp.bfloat16), jax.ShapeDtypeStruct((dec_rows, width), jnp.bfloat16),
                   *[jax.ShapeDtypeStruct((rows, keys.shape[0] * keys.shape[2]), jnp.bfloat16)] * 2,
                   jax.ShapeDtypeStruct((2, dec_rows * heads, head_dim), jnp.float32)),
        in_specs=[pl.BlockSpec(memory_space=pltpu.SMEM)] + [vmem] * 7 + [hbm] * 11,
        out_specs=(hbm, vmem, hbm, hbm, vmem),
        scratch_shapes=[
            pltpu.VMEM((2, 4 * per, WIRE_ROWS, WIRE), jnp.float32),
            pltpu.VMEM((2, 4 * per, WIRE_ROWS, WIRE), jnp.float32),
            pltpu.VMEM((2, 4 * per, WIRE_ROWS, WIRE), jnp.bfloat16),
            pltpu.VMEM((2, 2, dec_rows, mid), jnp.float32),
            pltpu.VMEM((2, 2, dec_rows, mid), jnp.float32),
            pltpu.VMEM((2, 2, dec_rows, mid), jnp.bfloat16),
            pltpu.VMEM((HALF_ROWS, width), jnp.bfloat16),
            pltpu.VMEM((n_up, HALF_ROWS, COLS), jnp.bfloat16),
            pltpu.VMEM((dec_rows, width), jnp.bfloat16),
            pltpu.VMEM((n_up, dec_rows, COLS), jnp.bfloat16),
            pltpu.VMEM((RING, 2, COLS, width), jnp.bfloat16),
            pltpu.VMEM((RING, ffn, 512), jnp.bfloat16),
            dma((2,)), dma((2, 4 * per)), dma((2,)), dma((2, 4 * per)),
            dma((2, 2)), dma((2, 2)), dma((2, 2)), dma((2, 2)),
            dma((RING,)), dma((RING,)), dma((2,)), dma((2, 4)), dma((2, 4)),
            pltpu.VMEM((2,) + k_cache.shape[1:], jnp.bfloat16),
            pltpu.VMEM((2,) + k_cache.shape[1:], jnp.bfloat16),
            pltpu.VMEM((RING, 2048, wqkv_b.shape[1]), jnp.bfloat16),
            pltpu.VMEM((width * heads // 256 * dec_rows, 256), jnp.float32),
            pltpu.VMEM((dec_rows * heads, wqkv_b.shape[1]), jnp.float32),
            pltpu.VMEM((3, dec_rows * heads, head_dim), jnp.float32),
            pltpu.VMEM((dec_rows, heads, head_dim), jnp.float32),
            dma((2,)), dma((2,)), dma((RING,)),
        ],
        compiler_params=pltpu.CompilerParams(collective_id=0, has_side_effects=True, vmem_limit_bytes=62 * 1024 * 1024),
        cost_estimate=pl.CostEstimate(flops=weights * (rows + dec_rows) // 2, bytes_accessed=weights * 3, transcendentals=0),
        name='block',
    )(c_len, x_rows, y_rows, attn_a, cos_tab, sin_tab, norm_a, norm_b, wo_a, wug_a, wd_a, wo_b, wug_b, wd_b, keys, vals, wqkv_b, k_cache, v_cache)


def front_kernel(s_len, qkv_a, cos_a, sin_a, k_cache, v_cache, attn_a, keys, vals, k_new, v_new, k_buf, v_buf, k_in, v_in, k_sem, v_sem):
    heads, rows, _ = qkv_a.shape
    head_dim = cos_a.shape[1]
    half = head_dim // 2
    dec_rows = k_cache.shape[0]
    n_tp = keys.shape[0]
    scale = head_dim ** -0.5

    def cache_in(b):
        return (pltpu.make_async_copy(k_cache.at[b], k_buf.at[b], k_in.at[b]), pltpu.make_async_copy(v_cache.at[b], v_buf.at[b], v_in.at[b]))

    def cache_out(b):
        return (pltpu.make_async_copy(k_buf.at[b], k_new.at[b], k_sem.at[b]), pltpu.make_async_copy(v_buf.at[b], v_new.at[b], v_sem.at[b]))

    for b in range(dec_rows):
        for copy in cache_in(b):
            copy.start()

    def rotate(val, cos_tab, sin_tab):
        val = val.astype(jnp.float32)
        swapped = jnp.concatenate([val[:, half:], val[:, :half]], axis=-1)
        return (val * cos_tab + swapped * sin_tab).astype(jnp.bfloat16)

    row = lax.broadcasted_iota(jnp.int32, (rows, rows), 0)
    col = lax.broadcasted_iota(jnp.int32, (rows, rows), 1)
    allowed = (col <= row) & (col < s_len[0])
    valid = lax.broadcasted_iota(jnp.int32, (rows, head_dim), 0) < s_len[0]
    zero = jnp.zeros((rows, head_dim), jnp.float32)
    dims = (((1,), (1,)), ((), ()))
    for h in range(heads):
        query = rotate(qkv_a[h, :, :head_dim], cos_a[...], sin_a[...])
        key = rotate(qkv_a[h, :, head_dim:2 * head_dim], cos_a[...], sin_a[...])
        val = qkv_a[h, :, 2 * head_dim:]
        place = pl.ds((h // n_tp) * head_dim, head_dim)
        keys[h % n_tp, :, place] = jnp.where(valid, key.astype(jnp.float32), zero).astype(jnp.bfloat16)
        vals[h % n_tp, :, place] = jnp.where(valid, val.astype(jnp.float32), zero).astype(jnp.bfloat16)
        scores = lax.dot_general(query, key, dims, preferred_element_type=jnp.float32) * scale
        scores = jnp.where(allowed, scores, -1e30)
        expd = jnp.exp(scores - jnp.max(scores, axis=-1, keepdims=True))
        prob = (expd / jnp.sum(expd, axis=-1, keepdims=True)).astype(jnp.bfloat16)
        attn_a[:, h * head_dim:(h + 1) * head_dim] = jnp.dot(prob, val, preferred_element_type=jnp.float32).astype(jnp.bfloat16)
        for b in range(h * dec_rows // heads, (h + 1) * dec_rows // heads):
            for copy in cache_in(b):
                copy.wait()
            for copy in cache_out(b):
                copy.start()
    for b in range(dec_rows):
        for copy in cache_out(b):
            copy.wait()


def insert_kernel(c_len, fresh, y_in, hid_in, k_old, v_old, k_new, v_new, hid_out, y_out, row_buf, row_sem, hid_buf, in_sem, out_sem):
    dec_rows, heads, head_dim = row_buf.shape[1:]
    del k_old, v_old
    pieces = in_sem.shape[0]
    depth = hid_in.shape[0] // pieces

    def piece_in(i):
        return pltpu.make_async_copy(hid_in.at[pl.ds(i * depth, depth), :], hid_buf.at[pl.ds(i * depth, depth), :], in_sem.at[i])

    def piece_out(i):
        return pltpu.make_async_copy(hid_buf.at[pl.ds(i * depth, depth), :], hid_out.at[pl.ds(i * depth, depth), :], out_sem.at[i])
    for i in range(pieces):
        piece_in(i).start()
    y_out[...] = y_in[...]
    for which in range(2):
        for b in range(dec_rows):
            row_buf[which, b] = fresh[which, b * heads:(b + 1) * heads, :].astype(jnp.bfloat16)

    def copies(b):
        place = pl.ds(pl.multiple_of(c_len[b] * heads, heads), heads)
        return [pltpu.make_async_copy(row_buf.at[which, b], dst.at[b, place, :], row_sem.at[which, b]) for which, dst in enumerate((k_new, v_new))]
    for b in range(dec_rows):
        for copy in copies(b):
            copy.start()
    for i in range(pieces):
        piece_in(i).wait()
        piece_out(i).start()
    for b in range(dec_rows):
        for copy in copies(b):
            copy.wait()
    for i in range(pieces):
        piece_out(i).wait()


def insert_call(c_len, fresh, y_in, hid_in, k_copy, v_copy):
    dec_rows = k_copy.shape[0]
    head_dim = k_copy.shape[2]
    heads = fresh.shape[1] // dec_rows
    hbm = pl.BlockSpec(memory_space=pl.ANY)
    vmem = pl.BlockSpec(memory_space=pltpu.VMEM)
    return pl.pallas_call(
        insert_kernel,
        out_shape=(jax.ShapeDtypeStruct(k_copy.shape, k_copy.dtype),) * 2 + (jax.ShapeDtypeStruct(hid_in.shape, hid_in.dtype), jax.ShapeDtypeStruct(y_in.shape, y_in.dtype)),
        in_specs=[pl.BlockSpec(memory_space=pltpu.SMEM), vmem, vmem, hbm, hbm, hbm],
        out_specs=(hbm, hbm, hbm, vmem),
        scratch_shapes=[pltpu.VMEM((2, dec_rows, heads, head_dim), jnp.bfloat16), pltpu.SemaphoreType.DMA((2, dec_rows)),
                        pltpu.VMEM(hid_in.shape, hid_in.dtype), pltpu.SemaphoreType.DMA((4,)), pltpu.SemaphoreType.DMA((4,))],
        input_output_aliases={4: 0, 5: 1},
        compiler_params=pltpu.CompilerParams(vmem_limit_bytes=62 * 1024 * 1024),
        name='insert',
    )(c_len, fresh, y_in, hid_in, k_copy, v_copy)


def rope_tables(count, head_dim):
    half_dim = head_dim // 2
    inv_freq = np.float32(ROPE_BASE) ** (-np.arange(half_dim, dtype=np.float32) / np.float32(half_dim))
    angles = np.arange(count, dtype=np.float32)[:, None] * inv_freq.astype(np.float32)[None, :]
    cos_tab, sin_tab = np.cos(angles.astype(np.float64)), np.sin(angles.astype(np.float64))
    both = np.concatenate([cos_tab, cos_tab], axis=-1), np.concatenate([-sin_tab, sin_tab], axis=-1)
    return tuple(jnp.asarray(tab.astype(np.float32)) for tab in both)


def front_call(x_rows, s_len, w_qkv_a, gain_a, k_cache, v_cache, cos_a, sin_a, tp_size):
    num_rows, width = x_rows.shape
    heads, wide = w_qkv_a.shape[1:]
    dec_rows, cache_rows, head_dim = k_cache.shape
    qkv_a = jnp.einsum('sd,dhe->she', rms_norm(x_rows, gain_a), w_qkv_a, preferred_element_type=jnp.float32).astype(jnp.bfloat16)
    qkv_a = jnp.transpose(qkv_a, (1, 0, 2))
    vmem = pl.BlockSpec(memory_space=pltpu.VMEM)
    hbm = pl.BlockSpec(memory_space=pl.ANY)
    dma = pltpu.SemaphoreType.DMA
    bf16 = jnp.bfloat16
    cache = jax.ShapeDtypeStruct((dec_rows, cache_rows, head_dim), bf16)
    moved = jax.ShapeDtypeStruct((tp_size, num_rows, heads // tp_size * head_dim), bf16)
    return pl.pallas_call(
        front_kernel,
        out_shape=(jax.ShapeDtypeStruct((num_rows, heads * head_dim), bf16), moved, moved, cache, cache),
        in_specs=[pl.BlockSpec(memory_space=pltpu.SMEM)] + [vmem] * 3 + [hbm] * 2,
        out_specs=(vmem, vmem, vmem, hbm, hbm),
        scratch_shapes=[pltpu.VMEM(cache.shape, bf16)] * 2 + [dma((dec_rows,))] * 4,
        compiler_params=pltpu.CompilerParams(vmem_limit_bytes=62 * 1024 * 1024),
        cost_estimate=pl.CostEstimate(flops=8 * num_rows * num_rows * heads * head_dim, bytes_accessed=8 * k_cache.size, transcendentals=0),
        name='front',
    )(s_len, qkv_a, cos_a, sin_a, k_cache, v_cache)


def solution(mesh):
    tp_size = mesh.shape['tp']
    side_size = mesh.shape['side']
    rows_spec = P(('pair', 'side'), None)
    flat_spec = P(('pair', 'side'))
    cache_spec = P(None, ('pair', 'side'), None, None, 'tp', None)
    prompt_spec = P(None, ('pair', 'side'), None, 'tp', None)
    in_specs = (rows_spec, flat_spec, rows_spec, cache_spec, cache_spec, flat_spec,
                P(None, None, 'tp', None), P(None, 'tp', None, None), P(None, None, None, 'tp'), P(None, 'tp', None), P(),
                P(None, None, None, 'tp', None), P(None, None, 'tp', None, None), P(None, None, None, 'tp'), P(None, 'tp', None), P())
    out_specs = (rows_spec, rows_spec, prompt_spec, prompt_spec, cache_spec, cache_spec)

    def body(x_prompt, s_len, y_tok, k_cache, v_cache, c_len, wqkv_a, wo_a, wug_a, wd_a, norm_a, wqkv_b, wo_b, wug_b, wd_b, norm_b):
        width = x_prompt.shape[1]
        head_dim = k_cache.shape[-1]
        dec_rows, slots, heads = k_cache.shape[1:4]
        k_rows = k_cache.reshape(dec_rows, slots * heads, head_dim)
        v_rows = v_cache.reshape(dec_rows, slots * heads, head_dim)
        cos_tab, sin_tab = rope_tables(max(slots, x_prompt.shape[0]), head_dim)
        attn_a, keys, vals, k_copy, v_copy = front_call(x_prompt, s_len, wqkv_a[0], norm_a[0, 0], k_rows, v_rows, cos_tab, sin_tab, tp_size)
        hidden, y_out, k_prompt, v_prompt, fresh = block_call(
            c_len, x_prompt, y_tok, attn_a, cos_tab, sin_tab, norm_a[0], norm_b[0],
            wo_a[0].reshape(-1, width), jnp.transpose(wug_a[0], (1, 2, 0)), wd_a[0],
            wo_b[0].reshape(-1, width), jnp.transpose(wug_b[0], (1, 2, 0)), wd_b[0], keys, vals,
            wqkv_b.reshape(width * heads, -1), k_rows, v_rows)
        k_new, v_new, hidden, y_out = insert_call(c_len, fresh, y_out, hidden, k_copy, v_copy)
        prompt_shape = (1, x_prompt.shape[0], heads, 1, head_dim)
        return (hidden, y_out, k_prompt.reshape(prompt_shape), v_prompt.reshape(prompt_shape),
                k_new.reshape(k_cache.shape), v_new.reshape(v_cache.shape))

    return jax.shard_map(body, mesh=mesh, in_specs=in_specs, out_specs=out_specs, check_vma=False)
```
